512 devices in a mesh: seq: 32 (over z, core), head: 16 (over y, x).
Axes of the slice: x: 4, y: 4, z: 16, core: 2. Of those that a mesh axis runs over, the one named last changes fastest.
Arguments:
- queries: bfloat16 [65536, 16, 128], P(('seq', 'head')), may hold values from -6 to 6
- keys: bfloat16 [65536, 16, 128], P(('seq', 'head')), may hold values from -6 to 6
- values: bfloat16 [65536, 16, 128], P(('seq', 'head')), may hold values from -6 to 6
- beta: float32 [65536, 16], P(('seq', 'head')), may hold values from 0 to 1
- log_decay: float32 [65536, 16], P(('seq', 'head')), may hold values from -1 to 0
- out_gate: bfloat16 [65536, 16, 128], P(('seq', 'head')), may hold values from -6 to 6
- norm_gain: float32 [128], replicated, may hold values from 0.1 to 1.9
Outputs:
- gated_out: bfloat16 [65536, 16, 128], P('seq', 'head')
The draws below stay inside these ranges and needn't reach their ends.
All inputs are finite; a program needn't handle non-finite values.
Results may differ from the reference program's by a relative error of at most 0.001.
Values may be sent and summed in bfloat16 or wider, within the bound.
No kernel may reach another device: no remote copies, remote signals or barrier semaphores. Data moves between devices by JAX's collectives and lax.ppermute only.
A program may use at most 64 MiB of HBM per device.

```python
import jax
import jax.numpy as jnp
from jax import lax

HK = 16
HV = 16
DK = 128
DV = 128
BLOCK = 128
TOK_DEV = 128
PROMPT_LENGTH = 65536


def head_kinds(key):
    slow_share = 5
    return jax.random.randint(jax.random.fold_in(key, 7), (HV,), 0, 10) < slow_share


def draw_beta(key, part):
    slow_heads = head_kinds(key)
    key_one, key_two, key_three = jax.random.split(jax.random.fold_in(key, 21), 3)
    lowest = 0.5 * DK / PROMPT_LENGTH
    slow_level = lowest * jnp.exp(jax.random.uniform(key_one, (HV,), minval=0.0, maxval=jnp.log(2.0)))
    fast_level = jnp.exp(jax.random.uniform(key_two, (HV,), minval=jnp.log(0.05), maxval=jnp.log(0.9)))
    head_level = jnp.where(slow_heads, slow_level, fast_level)
    roughness_measure = jax.random.uniform(key_three, (PROMPT_LENGTH, HV), minval=0.5, maxval=1.0)
    return (head_level[None, :] * roughness_measure).astype(jnp.float32)


def draw_log_decay(key, part):
    slow_heads = head_kinds(key)
    key_one, key_two, key_three, key_four, random_seed_five, random_seed_six = jax.random.split(jax.random.fold_in(key, 33), 6)
    slow_rate = 0.1 / PROMPT_LENGTH * jnp.exp(jax.random.uniform(key_one, (HV,), minval=0.0, maxval=jnp.log(5.0)))
    fast_rate = jnp.exp(jax.random.uniform(key_two, (HV,), minval=jnp.log(0.02), maxval=jnp.log(0.05)))
    steady_speed = jnp.where(slow_heads, slow_rate, fast_rate)
    roughness_measure = jnp.exp(jax.random.uniform(key_three, (PROMPT_LENGTH, HV), minval=jnp.log(0.5), maxval=jnp.log(2.0)))
    shard_division = jnp.exp(jax.random.uniform(key_four, (PROMPT_LENGTH // TOK_DEV, 1), minval=jnp.log(0.5), maxval=jnp.log(2.0)))
    shard_division = jnp.repeat(shard_division, TOK_DEV, axis=0)
    spike_location = jax.random.randint(random_seed_five, (6,), 0, PROMPT_LENGTH)
    spike_height = jax.random.uniform(random_seed_six, (6,), minval=0.2, maxval=0.7)
    spike_influence = lax.broadcasted_iota(jnp.int32, (PROMPT_LENGTH, 6), 0) == spike_location[None, :]
    spike_charge = jnp.minimum(jnp.sum(jnp.where(spike_influence, spike_height[None, :], 0.0), axis=1), 0.7)
    overall_summation = -(steady_speed[None, :] * roughness_measure * shard_division) - spike_charge[:, None]
    return jnp.maximum(overall_summation, -1.0).astype(jnp.float32)


def level_of(stream_key, shape, shards, low, high):
    def one(position, parts):
        heights = jax.random.uniform(jax.random.fold_in(jax.random.fold_in(stream_key, 6), position), (parts,), jnp.float32, low / len(shards), high / len(shards))
        return jnp.repeat(jnp.exp(heights), shape[position] // parts).reshape((-1,) + (1,) * (len(shape) - position - 1))

    gain = one(*shards[0])
    for cut in shards[1:]:
        gain = gain * one(*cut)
    return gain


def scatter_about(own_key, dims, scale, limit, shards=(), kind=jnp.bfloat16):
    gain = level_of(own_key, dims, shards, -0.22, 0.18) if shards else 1.0
    entries = jax.random.normal(own_key, dims, jnp.float32) * scale * gain
    return jnp.minimum(jnp.maximum(entries, -limit), limit).astype(kind)


def setup_inputs(seed: int = 0) -> dict:
    seeds = jax.random.split(jax.random.key(seed), 8)
    return {
        "queries": scatter_about(seeds[0], (PROMPT_LENGTH, HK, DK), 1.0, 6.0, ((0, 512),)),
        "keys": scatter_about(seeds[1], (PROMPT_LENGTH, HK, DK), 1.0, 6.0, ((0, 512),)),
        "values": scatter_about(seeds[2], (PROMPT_LENGTH, HV, DV), 1.0, 6.0, ((0, 512),)),
        "beta": draw_beta(jax.random.fold_in(seeds[7], 71), 0),
        "log_decay": draw_log_decay(jax.random.fold_in(seeds[7], 71), 0),
        "out_gate": scatter_about(seeds[5], (PROMPT_LENGTH, HV, DV), 1.0, 6.0, ((0, 512),)),
        "norm_gain": jnp.clip(1.0 + 0.18 * jax.random.normal(seeds[6], (DV,), jnp.float32), 0.1, 1.9),
    }


HIGHEST_PREC = lax.Precision.HIGHEST

def unit_rows(matrix):
    return matrix * lax.rsqrt(lax.optimization_barrier(jnp.sum(matrix * matrix, axis=-1, keepdims=True)) + 1e-06)

def block_terms(query_block, key_block, value_block, beta_block, decay_block):
    key_dim = query_block.shape[-1]
    copies = value_block.shape[1] // query_block.shape[1]
    length = query_block.shape[0]
    query_unit = unit_rows(query_block.astype(jnp.float32)) * key_dim ** (-0.5)
    key_unit = unit_rows(key_block.astype(jnp.float32))
    query_heads = jnp.transpose(jnp.repeat(query_unit, copies, axis=1), (1, 0, 2))
    key_heads = jnp.transpose(jnp.repeat(key_unit, copies, axis=1), (1, 0, 2))
    value_heads = jnp.transpose(value_block.astype(jnp.float32), (1, 0, 2))
    beta_rows = jnp.transpose(beta_block)
    cumulative = jnp.cumsum(jnp.transpose(decay_block), axis=1)
    row_ids = lax.broadcasted_iota(jnp.int32, (length, length), 0)
    col_ids = lax.broadcasted_iota(jnp.int32, (length, length), 1)
    inclusive = row_ids >= col_ids
    strict = row_ids > col_ids
    spread = cumulative[:, :, None] - cumulative[:, None, :]
    fading = jnp.where(inclusive, jnp.exp(jnp.where(inclusive, spread, 0.0)), 0.0)
    key_key = jnp.einsum('hid,hjd->hij', key_heads, key_heads, precision=HIGHEST_PREC)
    query_key = jnp.einsum('hid,hjd->hij', query_heads, key_heads, precision=HIGHEST_PREC)
    unit_lower = jnp.where(strict, beta_rows[:, :, None] * fading * key_key, 0.0) + jnp.eye(length, dtype=jnp.float32)
    growth = jnp.exp(cumulative)
    right_cols = jnp.concatenate([(beta_rows * growth)[:, :, None] * key_heads, beta_rows[:, :, None] * value_heads], axis=2)
    solved = lax.linalg.triangular_solve(unit_lower, right_cols, left_side=True, lower=True, unit_diagonal=True)
    weighted_keys = solved[:, :, :key_dim]
    base_values = solved[:, :, key_dim:]
    mixing = fading * query_key
    query_reach = growth[:, :, None] * query_heads - jnp.einsum('hij,hjd->hid', mixing, weighted_keys, precision=HIGHEST_PREC)
    local_rows = jnp.einsum('hij,hjv->hiv', mixing, base_values, precision=HIGHEST_PREC)
    tail_fade = jnp.exp(cumulative[:, -1:] - cumulative)
    tail_keys = tail_fade[:, :, None] * key_heads
    carry_map = growth[:, -1][:, None, None] * jnp.eye(key_dim, dtype=jnp.float32) - jnp.einsum('hcd,hce->hde', weighted_keys, tail_keys, precision=HIGHEST_PREC)
    offset = jnp.einsum('hcv,hcd->hvd', base_values, tail_keys, precision=HIGHEST_PREC)
    return (local_rows, query_reach, carry_map, offset)

def gated_norm(results, out_gate, norm_gain):
    norm_scale = lax.rsqrt(lax.optimization_barrier(jnp.mean(results * results, axis=-1, keepdims=True)) + 1e-06)
    gate_f32 = out_gate.astype(jnp.float32)
    return (results * norm_scale * norm_gain * jax.nn.silu(gate_f32)).astype(jnp.bfloat16)

def reference(queries, keys, values, beta, log_decay, out_gate, norm_gain):
    blocks = queries.shape[0] // BLOCK

    def to_blocks(array):
        return array.reshape((blocks, BLOCK) + array.shape[1:])

    def advance(state_now, pieces):
        local_rows, query_reach, carry_map, offset = block_terms(*pieces)
        results = local_rows + jnp.einsum('hcd,hvd->hcv', query_reach, state_now, precision=HIGHEST_PREC)
        state_next = jnp.einsum('hvd,hde->hve', state_now, carry_map, precision=HIGHEST_PREC) + offset
        return (state_next, jnp.transpose(results, (1, 0, 2)))
    initial = jnp.zeros((HV, DV, DK), jnp.float32)
    pieces = (to_blocks(queries), to_blocks(keys), to_blocks(values), to_blocks(beta), to_blocks(log_decay))
    _, results = lax.scan(advance, initial, pieces)
    results = results.reshape((queries.shape[0], HV, DV))
    return gated_norm(results, out_gate, norm_gain)
```

```python
import jax
import jax.numpy as jnp
from jax import lax
from jax.experimental import pallas as pl
from jax.experimental.pallas import tpu as pltpu
from jax.sharding import Mesh
from jax.sharding import PartitionSpec as P


F32 = jnp.float32
BF16 = jnp.bfloat16
N = 128
EPS = 1e-06
SUB = 16


def dot(a, b):
    return jnp.dot(a, b, preferred_element_type=F32)


def dot_nt(a, b):
    return lax.dot_general(a, b, (((1,), (1,)), ((), ())), preferred_element_type=F32)


def split2(x):
    high = x.astype(BF16)
    return high, (x - high.astype(F32)).astype(BF16)


def lanes(*parts):
    return jnp.concatenate(parts, axis=1)


def rows(*parts):
    return jnp.concatenate(parts, axis=0)


def square_mm(a_parts, b_parts):
    b_both = lanes(*b_parts)
    both = dot(lanes(*a_parts), rows(b_both, b_both))
    return both[:, :N] + both[:, N:]


def wide_mm(a_parts, b_high, b_low):
    return dot(lanes(*a_parts), rows(b_high, b_high)) + dot(a_parts[0], b_low)


def compose(later, earlier):
    high, low = split2(earlier)
    out = wide_mm(split2(later[:, :N]), high, low)
    return out + lanes(jnp.zeros((N, N), F32), later[:, N:])


def iotas():
    return lax.broadcasted_iota(jnp.int32, (N, N), 0), lax.broadcasted_iota(jnp.int32, (N, N), 1)


def terms_kernel(kv_ref, en_ref, grow_ref, wu_hi_ref, wu_lo_ref, pair_ref, total_ref):
    blocks = kv_ref.shape[0]
    r, c = iotas()
    one = lambda cond: cond.astype(F32).astype(BF16)
    lower = one(r >= c)
    eye16 = one(r == c)
    eye = (r == c).astype(F32)
    inclusive = r >= c
    picks = lanes(one(r > c), jnp.ones((N, N), BF16))
    picks = rows(picks, picks, picks)
    lane16 = lax.broadcasted_iota(jnp.int32, (SUB, N), 1)
    row16 = lax.broadcasted_iota(jnp.int32, (SUB, N), 0)
    start16 = (row16 == lane16 % SUB).astype(F32)
    base16 = lane16 // SUB * SUB
    merge_masks = [one((r // m == c // m + 1) & (c // m % 2 == 0)) for m in (16, 32, 64)]
    group = range(blocks)

    keys = [kv_ref[b, :N, :N] for b in group]
    kk = [dot_nt(k, k) for k in keys]
    aux = [kv_ref[b, N : N + 16, :] for b in group]

    def sums(a):
        left = [rows(lower * a[i : i + 1, :N], eye16 * a[i : i + 1, N:]) for i in range(3)]
        return dot(lanes(*left), picks)

    summed = [sums(a) for a in aux]
    fade = [jnp.exp(s[:N, :N]) for s in summed]
    cum = [s[:N, N:] for s in summed]
    beta_low = [s[N:, :N] for s in summed]
    beta_row = []
    cum_row = []
    for b in group:
        a = aux[b][:8].astype(F32)
        beta_row.append(a[0:1, N:] + a[1:2, N:] + a[2:3, N:])
        cum_row.append(jnp.sum(eye * cum[b], axis=0, keepdims=True))
    diag = [eye * x for x in kk]
    nk_row = [lax.rsqrt(jnp.sum(d, axis=0, keepdims=True) + EPS) for d in diag]
    nk_col = [lax.rsqrt(jnp.sum(d, axis=1, keepdims=True) + EPS) for d in diag]
    low = []
    for b in group:
        fade_n = fade[b] * nk_row[b]
        en_ref[b] = jnp.where(inclusive, fade_n, 0.0)
        low.append(beta_low[b] * fade_n * (nk_col[b] * kk[b]))
        grow_ref[b] = jnp.exp(cum[b])
    inv = []
    for b in group:
        small = sum(
            jnp.where(lane16 // SUB == s, low[b][SUB * s : SUB * (s + 1)], 0.0) for s in range(N // SUB)
        )
        x = start16
        for j in range(SUB - 1):
            col = jnp.take_along_axis(small, base16 + j, axis=1)
            x = x - col * x[j : j + 1, :]
        inv.append(rows(*[jnp.where(lane16 // SUB == s, x, 0.0) for s in range(N // SUB)]))
    low_parts = [split2(x) for x in low]
    for mask in merge_masks:
        parts = [split2(x) for x in inv]
        left = [square_mm(parts[b], [p * mask for p in low_parts[b]]) for b in group]
        left = [split2(x) for x in left]
        inv = [inv[b] - square_mm(left[b], parts[b]) for b in group]
    pairs = []
    for b in group:
        grow_row = jnp.exp(cum_row[b])
        for_u = inv[b] * beta_row[b]
        for_w = for_u * (grow_row * nk_row[b])
        value = kv_ref[b, :N, N:]
        w = dot(lanes(*split2(for_w)), rows(keys[b], keys[b]))
        u = dot(lanes(*split2(for_u)), rows(value, value))
        wu = lanes(w, u)
        wu_hi_ref[b], wu_lo_ref[b] = split2(wu)
        total = cum[b][N - 1 : N, :]
        tail = jnp.exp(total - cum[b]) * nk_col[b]
        high, lo = split2(wu * lanes(tail, tail))
        key_t = keys[b].T
        out = dot(lanes(key_t, key_t), rows(high, lo))
        pair = lanes(eye * jnp.exp(total) - out[:, :N], out[:, N:])
        pair_ref[b] = pair
        pairs.append(pair)
    while len(pairs) > 1:
        pairs = [compose(pairs[i + 1], pairs[i]) for i in range(0, len(pairs), 2)]
    total_ref[...] = pairs[0]


def reach_kernel(kv_ref, q_ref, en_ref, grow_ref, wu_hi_ref, wu_lo_ref, pair_ref, r0_ref, hi_ref, lo_ref):
    blocks = kv_ref.shape[0]
    r, c = iotas()
    group = range(blocks)
    carried = [lanes((r == c).astype(F32), jnp.zeros((N, N), F32))]
    for b in range(blocks - 1):
        carried.append(compose(pair_ref[b], carried[b]))
    for b in group:
        q = q_ref[b, :, :N]
        mixing = en_ref[b] * dot_nt(q, kv_ref[b, :N, :N])
        mixed = wide_mm(split2(mixing), wu_hi_ref[b], wu_lo_ref[b])
        q32 = q.astype(F32)
        reach = grow_ref[b] * q32 - mixed[:, :N]
        high, lo = split2(carried[b])
        out = wide_mm(split2(reach), high, lo)
        scale = lax.rsqrt(jnp.sum(q32 * q32, axis=1, keepdims=True) + EPS) * N**-0.5
        r0_ref[b] = (mixed[:, N:] + out[:, N:]) * scale
        hi_ref[b], lo_ref[b] = split2(out[:, :N] * scale)


def compose_kernel(later_ref, earlier_ref, out_ref):
    out_ref[...] = compose(later_ref[...], earlier_ref[...])


def finish_kernel(flag_ref, r0_ref, hi_ref, lo_ref, near_ref, far_ref, own_ref, gate_ref, gain_ref, out_ref):
    def apply(pair, state):
        return square_mm(split2(pair[:, :N]), split2(state)) + pair[:, N:]

    state = apply(near_ref[...], far_ref[...])
    state = jnp.where(flag_ref[0] == 0, state, apply(own_ref[...], state))
    y_both = lanes(*split2(state))
    y_both = rows(y_both, y_both)
    for b in range(r0_ref.shape[0]):
        both = dot(lanes(hi_ref[b], lo_ref[b]), y_both)
        res = r0_ref[b] + both[:, :N] + both[:, N:]
        norm = lax.rsqrt(jnp.mean(res * res, axis=1, keepdims=True) + EPS)
        gate = gate_ref[b, :, N:].astype(F32)
        silu = gate / (1.0 + jnp.exp(-gate))
        out_ref[b] = (res * norm * gain_ref[...] * silu).astype(BF16)


def call(kernel, out_shape, name, **kw):
    return pl.pallas_call(
        kernel,
        out_shape=out_shape,
        name=name,
        compiler_params=pltpu.CompilerParams(vmem_limit_bytes=56 * 2**20),
        **kw,
    )


def shape(*dims, dtype=F32):
    return jax.ShapeDtypeStruct(dims, dtype)


def parts3(x):
    high = lax.reduce_precision(x, 8, 7)
    rest = x - high
    mid = lax.reduce_precision(rest, 8, 7)
    return [p.astype(BF16) for p in (high, mid, rest - mid)]


def by_head(array):
    return jnp.transpose(array, (1, 0, 2))


def to_heads(array):
    return lax.all_to_all(array, "head", split_axis=0, concat_axis=0, tiled=True)


def body(queries, keys, values, beta, log_decay, out_gate, norm_gain):
    heads = values.shape[1]
    z = lax.axis_size("z")
    decay_parts = parts3(jnp.transpose(log_decay))
    beta_parts = parts3(jnp.transpose(beta))
    aux = jnp.concatenate(
        [jnp.stack(decay_parts, axis=1), jnp.stack(beta_parts, axis=1)], axis=2
    )
    aux = jnp.pad(aux, ((0, 0), (0, 13), (0, 0)))
    kv = jnp.concatenate([by_head(keys), by_head(values)], axis=2)
    kv = to_heads(jnp.concatenate([kv, aux], axis=1))
    qg = jnp.concatenate([by_head(queries), by_head(out_gate)], axis=2)
    qg = to_heads(qg)
    blocks = kv.shape[0]
    cube = shape(blocks, N, N)
    wide16 = shape(blocks, N, 2 * N, dtype=BF16)
    en, grow, wu_hi, wu_lo, pairs, total = call(
        terms_kernel,
        (cube, cube, wide16, wide16, shape(blocks, N, 2 * N), shape(N, 2 * N)),
        "terms",
    )(kv)
    join = call(compose_kernel, shape(N, 2 * N), "join")
    core = lax.axis_index("c")
    partner = lax.ppermute(total, "c", [(0, 1), (1, 0)])
    first = jnp.where(core == 0, total, partner)
    second = jnp.where(core == 0, partner, total)
    window = join(second, first)

    def up(x, d):
        return lax.ppermute(x, "z", [(i, i + d) for i in range(z - d)])

    span = 1
    while span * 2 < z:
        window = join(window, up(window, span))
        span *= 2
    near = up(window, 1)
    far = up(window[:, N:], span + 1)
    r0, r1_hi, r1_lo = call(
        reach_kernel,
        (cube, shape(blocks, N, N, dtype=BF16), shape(blocks, N, N, dtype=BF16)),
        "reach",
    )(kv, qg, en, grow, wu_hi, wu_lo, pairs)
    vmem = pl.BlockSpec(memory_space=pltpu.VMEM)
    out = call(
        finish_kernel,
        shape(blocks, N, N, dtype=BF16),
        "finish",
        in_specs=[pl.BlockSpec(memory_space=pltpu.SMEM)] + [vmem] * 8,
        out_specs=vmem,
    )(core.reshape(1).astype(jnp.int32), r0, r1_hi, r1_lo, near, far, first, qg, norm_gain.reshape(1, N))
    return out.reshape(blocks * N, 1, N)


def solution(mesh):
    finer = Mesh(mesh.devices.reshape(-1, 2, mesh.shape["head"]), ("z", "c", "head"))
    tokens = ("z", "c", "head")
    in_specs = (
        P(tokens, None, None),
        P(tokens, None, None),
        P(tokens, None, None),
        P(tokens, None),
        P(tokens, None),
        P(tokens, None, None),
        P(),
    )
    out_specs = P(("z", "c"), "head", None)
    return jax.shard_map(body, mesh=finer, in_specs=in_specs, out_specs=out_specs, check_vma=False)
```

```python
import jax
import jax.numpy as jnp
from jax import lax
from jax.experimental import pallas as pl
from jax.experimental.pallas import tpu as pltpu
from jax.sharding import Mesh
from jax.sharding import PartitionSpec as P


F32 = jnp.float32
BF16 = jnp.bfloat16
N = 128
EPS = 1e-06
SUB = 16


def dot(a, b):
    return jnp.dot(a, b, preferred_element_type=F32)


def dot_nt(a, b):
    return lax.dot_general(a, b, (((1,), (1,)), ((), ())), preferred_element_type=F32)


def split2(x):
    high = x.astype(BF16)
    return high, (x - high.astype(F32)).astype(BF16)


def lanes(*parts):
    return jnp.concatenate(parts, axis=1)


def rows(*parts):
    return jnp.concatenate(parts, axis=0)


def square_mm(a_parts, b_parts):
    b_both = lanes(*b_parts)
    both = dot(lanes(*a_parts), rows(b_both, b_both))
    return both[:, :N] + both[:, N:]


def wide_mm(a_parts, b_high, b_low):
    return dot(lanes(*a_parts), rows(b_high, b_high)) + dot(a_parts[0], b_low)


def compose(later, earlier):
    high, low = split2(earlier)
    out = wide_mm(split2(later[:, :N]), high, low)
    return out + lanes(jnp.zeros((N, N), F32), later[:, N:])


def iotas():
    return lax.broadcasted_iota(jnp.int32, (N, N), 0), lax.broadcasted_iota(jnp.int32, (N, N), 1)


def terms_kernel(core_ref, kv_ref, map_ref, off_ref, send_ref, *rest):
    outs, (en_ref, grow_ref, wu_hi_ref, wu_lo_ref, node_ref), sems = rest[:5], rest[5:10], rest[10]
    blocks = kv_ref.shape[0]
    copies = []

    def save(which, first=0, count=blocks):
        part = pl.ds(first, count)
        copies.append(
            pltpu.make_async_copy(rest[5 + which].at[part], outs[which].at[part], sems.at[len(copies)])
        )
        copies[-1].start()

    r, c = iotas()
    one = lambda cond: cond.astype(F32).astype(BF16)
    lower = one(r >= c)
    eye16 = one(r == c)
    eye = (r == c).astype(F32)
    inclusive = r >= c
    picks = lanes(one(r > c), jnp.ones((N, N), BF16))
    picks = rows(picks, picks, picks)
    lane16 = lax.broadcasted_iota(jnp.int32, (SUB, N), 1)
    row16 = lax.broadcasted_iota(jnp.int32, (SUB, N), 0)
    start16 = (row16 == lane16 % SUB).astype(F32)
    base16 = lane16 // SUB * SUB
    merge_masks = [one((r // m == c // m + 1) & (c // m % 2 == 0)) for m in (16, 32, 64)]
    group = range(blocks)

    keys = [kv_ref[b, :N, :N] for b in group]
    kk = [dot_nt(k, k) for k in keys]
    aux = [kv_ref[b, N : N + 8, :] for b in group]

    def sums(a):
        left = [rows(lower * a[i : i + 1, :N], eye16 * a[i : i + 1, N:]) for i in range(3)]
        return dot(lanes(*left), picks)

    summed = [sums(a) for a in aux]
    fade = [jnp.exp(s[:N, :N]) for s in summed]
    cum = [s[:N, N:] for s in summed]
    beta_low = [s[N:, :N] for s in summed]
    beta_row = []
    cum_row = []
    for b in group:
        a = aux[b][:8].astype(F32)
        beta_row.append(a[0:1, N:] + a[1:2, N:] + a[2:3, N:])
        cum_row.append(jnp.sum(eye * cum[b], axis=0, keepdims=True))
    diag = [eye * x for x in kk]
    nk_row = [lax.rsqrt(jnp.sum(d, axis=0, keepdims=True) + EPS) for d in diag]
    nk_col = [lax.rsqrt(jnp.sum(d, axis=1, keepdims=True) + EPS) for d in diag]
    low = []
    for b in group:
        fade_n = fade[b] * nk_row[b]
        en_ref[b] = jnp.where(inclusive, fade_n, 0.0)
        low.append(beta_low[b] * fade_n * (nk_col[b] * kk[b]))
        grow_ref[b] = jnp.exp(cum[b])
    save(0)
    save(1)
    inv = []
    for b in group:
        small = sum(
            jnp.where(lane16 // SUB == s, low[b][SUB * s : SUB * (s + 1)], 0.0) for s in range(N // SUB)
        )
        x = start16
        for j in range(SUB - 1):
            col = jnp.take_along_axis(small, base16 + j, axis=1)
            x = x - col * x[j : j + 1, :]
        inv.append(rows(*[jnp.where(lane16 // SUB == s, x, 0.0) for s in range(N // SUB)]))
    low_parts = [split2(x) for x in low]
    for mask in merge_masks:
        parts = [split2(x) for x in inv]
        left = [square_mm(parts[b], [p * mask for p in low_parts[b]]) for b in group]
        left = [split2(x) for x in left]
        inv = [inv[b] - square_mm(left[b], parts[b]) for b in group]
    pairs = []
    for b in group:
        grow_row = jnp.exp(cum_row[b])
        for_u = inv[b] * beta_row[b]
        for_w = for_u * (grow_row * nk_row[b])
        value = kv_ref[b, :N, N:]
        w = dot(lanes(*split2(for_w)), rows(keys[b], keys[b]))
        u = dot(lanes(*split2(for_u)), rows(value, value))
        wu = lanes(w, u)
        wu_hi_ref[b], wu_lo_ref[b] = split2(wu)
        total = cum[b][N - 1 : N, :]
        tail = jnp.exp(total - cum[b]) * nk_col[b]
        high, lo = split2(wu * lanes(tail, tail))
        key_t = keys[b].T
        out = dot(lanes(key_t, key_t), rows(high, lo))
        pair = lanes(eye * jnp.exp(total) - out[:, :N], out[:, N:])
        node_ref[b] = pair
        pairs.append(pair)
    save(2)
    save(3)
    save(4)
    spot = blocks
    while len(pairs) > 2:
        pairs = [compose(pairs[i + 1], pairs[i]) for i in range(0, len(pairs), 2)]
        for i, pair in enumerate(pairs):
            node_ref[spot + i] = pair
        save(4, spot, len(pairs))
        spot += len(pairs)
    total = compose(pairs[1], pairs[0])
    map_ref[...] = total[:, :N]
    off_ref[...] = total[:, N:]
    send_ref[...] = jnp.where(core_ref[0] == 0, total[:, N:], total[:, :N])
    for copy in copies:
        copy.wait()


def reach_kernel(kv_ref, q_ref, *rest):
    sources, (r0_ref, hi_ref, lo_ref) = rest[:5], rest[5:8]
    buffers, sems = rest[8:13], rest[13]
    blocks = kv_ref.shape[0]
    copies = [
        pltpu.make_async_copy(sources[i], buffers[i], sems.at[i]) for i in range(len(sources))
    ]
    for copy in copies:
        copy.start()
    node_ref, en_ref, grow_ref, wu_hi_ref, wu_lo_ref = buffers
    copies[0].wait()
    carried = {}
    base, width = {1: 0}, 1
    while width * 2 < blocks:
        base[width * 2] = base[width] + blocks // width
        width *= 2
    step = blocks // 2
    while step:
        for b in range(step, blocks, 2 * step):
            node = node_ref[base[step] + (b - step) // step]
            carried[b] = compose(node, carried[b - step]) if b > step else node
        step //= 2
    for copy in copies[1:]:
        copy.wait()
    for b in range(blocks):
        q = q_ref[b, :, :N]
        mixing = en_ref[b] * dot_nt(q, kv_ref[b, :N, :N])
        mixed = wide_mm(split2(mixing), wu_hi_ref[b], wu_lo_ref[b])
        q32 = q.astype(F32)
        scale = lax.rsqrt(jnp.sum(q32 * q32, axis=1, keepdims=True) + EPS) * N**-0.5
        reach = grow_ref[b] * q32 - mixed[:, :N]
        local = mixed[:, N:]
        if b:
            high, low = split2(carried[b])
            out = wide_mm(split2(reach), high, low)
            reach, local = out[:, :N], local + out[:, N:]
        r0_ref[b] = local * scale
        hi_ref[b], lo_ref[b] = split2(reach * scale)


def advance(left, right, extra):
    return square_mm(split2(left), split2(right)) + extra


def pair_kernel(core_ref, map_ref, off_ref, got_ref, out_ref):
    first = core_ref[0] == 0
    own = map_ref[...]
    got = got_ref[...]
    left = jnp.where(first, got, own)
    right = jnp.where(first, own, got)
    out_ref[...] = advance(left, right, jnp.where(first, 0.0, off_ref[...]))


def join_kernel(core_ref, near_ref, map_ref, far_ref, out_ref):
    first = core_ref[0] == 0
    near = near_ref[...]
    left = jnp.where(first, near, map_ref[...])
    out_ref[...] = advance(left, far_ref[...], jnp.where(first, 0.0, near))


def finish_kernel(core_ref, r0_ref, hi_ref, lo_ref, own_ref, swap_ref, far0_ref, far1_ref, map_ref, off_ref, gate_ref, gain_ref, out_ref):
    first = core_ref[0] == 0
    own = own_ref[...]
    swap = swap_ref[...]
    state = advance(
        jnp.where(first, own, swap), far0_ref[...] + far1_ref[...], jnp.where(first, swap, own)
    )
    state = jnp.where(first, state, advance(map_ref[...], state, off_ref[...]))
    y_both = lanes(*split2(state))
    y_both = rows(y_both, y_both)
    for b in range(r0_ref.shape[0]):
        both = dot(lanes(hi_ref[b], lo_ref[b]), y_both)
        res = r0_ref[b] + both[:, :N] + both[:, N:]
        norm = lax.rsqrt(jnp.mean(res * res, axis=1, keepdims=True) + EPS)
        gate = gate_ref[b, :, N:].astype(F32)
        silu = gate / (1.0 + jnp.exp(-gate))
        out_ref[b] = (res * norm * gain_ref[...] * silu).astype(BF16)


def call(kernel, out_shape, inputs, core=None, remote=(), spill=(), sems=0):
    vmem = pl.BlockSpec(memory_space=pltpu.VMEM)
    hbm = pl.BlockSpec(memory_space=pltpu.HBM)
    specs = [vmem] * len(inputs) + [hbm] * len(remote)
    inputs = [*inputs, *(pltpu.with_memory_space_constraint(a, pltpu.HBM) for a in remote)]
    if core is not None:
        specs = [pl.BlockSpec(memory_space=pltpu.SMEM)] + specs
        inputs = [core, *inputs]
    return pl.pallas_call(
        kernel,
        out_shape=[*out_shape, *(pltpu.HBM(o.shape, o.dtype) for o in spill)],
        in_specs=specs,
        out_specs=[vmem] * len(out_shape) + [hbm] * len(spill),
        scratch_shapes=[pltpu.VMEM(o.shape, o.dtype) for o in (*remote, *spill)]
        + ([pltpu.SemaphoreType.DMA((sems,))] if sems else []),
        compiler_params=pltpu.CompilerParams(vmem_limit_bytes=40 * 2**20),
    )(*inputs)


def near(*arrays):
    return [pltpu.with_memory_space_constraint(a, pltpu.VMEM) for a in arrays]


def kept(*dims, dtype=F32):
    return pltpu.VMEM(dims, dtype)


def shape(*dims, dtype=F32):
    return jax.ShapeDtypeStruct(dims, dtype)


def parts3(x):
    high = lax.reduce_precision(x, 8, 7)
    rest = x - high
    mid = lax.reduce_precision(rest, 8, 7)
    return [p.astype(BF16) for p in (high, mid, rest - mid)]


def by_head(array):
    return jnp.transpose(array, (1, 0, 2))


def to_heads(array):
    return lax.all_to_all(array, "head", split_axis=0, concat_axis=0, tiled=True)


def layer(queries, keys, values, beta, log_decay, out_gate, norm_gain):
    z = lax.axis_size("z")
    decay_parts = parts3(jnp.transpose(log_decay))
    beta_parts = parts3(jnp.transpose(beta))
    aux = jnp.concatenate(
        [jnp.stack(decay_parts, axis=1), jnp.stack(beta_parts, axis=1)], axis=2
    )
    aux = jnp.pad(aux, ((0, 0), (0, 5), (0, 0)))
    kv = jnp.concatenate([by_head(keys), by_head(values)], axis=2)
    kv = to_heads(jnp.concatenate([kv, aux], axis=1))
    qg = jnp.concatenate([by_head(queries), by_head(out_gate)], axis=2)
    blocks = kv.shape[0]
    cube = shape(blocks, N, N)
    square = kept(N, N)
    wide16 = shape(blocks, N, 2 * N, dtype=BF16)
    core = lax.axis_index("c").astype(jnp.int32).reshape(1)
    kv, qg = lax.optimization_barrier((kv, qg))
    own_map, own_off, send, en, grow, wu_hi, wu_lo, nodes = call(
        terms_kernel,
        [square] * 3,
        near(kv),
        core,
        spill=[cube, cube, wide16, wide16, shape(2 * blocks - 2, N, 2 * N)],
        sems=8,
    )
    swap = [(0, 1), (1, 0)]
    got = lax.ppermute(send, "c", swap)
    first_map = lax.ppermute(own_map, "c", [(0, 1)])
    chip = call(pair_kernel, [square], near(own_map, own_off, got), core)[0]

    def up(x, d):
        return lax.ppermute(x, "z", [(i, i + d) for i in range(z - d)])

    def cross(x, d, *routes):
        pairs = [
            (2 * i + source, 2 * (i + d) + target)
            for i in range(z - d)
            for source, target in zip(routes[::2], routes[1::2])
        ]
        return lax.ppermute(x, ("z", "c"), pairs)

    def join(one, maps, far):
        return call(join_kernel, [square], near(one, maps, far), core)[0]

    window, span = chip, 1
    while span * 2 < z:
        far = up(window, span)
        maps = lax.ppermute(window, "c", [(0, 1)])
        if span * 4 >= z:
            qg, maps = lax.optimization_barrier((qg, maps))
            qg = to_heads(qg)
        window = join(window, maps, far)
        span *= 2
    qg, window = lax.optimization_barrier((qg, window))
    far0 = cross(window, span + 1, 1, 0)
    far1 = cross(window, span + 1, 1, 1)
    own = up(window, 1)
    other = cross(window, 1, 0, 1, 1, 0)
    half = kept(blocks, N, N, dtype=BF16)
    r0, r1_hi, r1_lo = call(
        reach_kernel,
        [kept(blocks, N, N), half, half],
        near(kv, qg),
        remote=[nodes, en, grow, wu_hi, wu_lo],
        sems=5,
    )
    (out,) = call(
        finish_kernel,
        [shape(blocks, N, N, dtype=BF16)],
        near(r0, r1_hi, r1_lo, own, other, far0, far1, first_map, got)
        + [qg, norm_gain.reshape(1, N)],
        core,
    )
    return out.reshape(blocks * N, 1, N)


def solution(mesh):
    finer = Mesh(mesh.devices.reshape(-1, 2, mesh.shape["head"]), ("z", "c", "head"))
    tokens = ("z", "c", "head")
    in_specs = (
        P(tokens, None, None),
        P(tokens, None, None),
        P(tokens, None, None),
        P(tokens, None),
        P(tokens, None),
        P(tokens, None, None),
        P(),
    )
    out_specs = P(("z", "c"), "head", None)
    return jax.shard_map(layer, mesh=finer, in_specs=in_specs, out_specs=out_specs, check_vma=False)
```

```python
import jax
import jax.numpy as jnp
from jax import lax
from jax.experimental import pallas as pl
from jax.experimental.pallas import tpu as pltpu
from jax.sharding import Mesh
from jax.sharding import PartitionSpec as P


F32 = jnp.float32
BF16 = jnp.bfloat16
N = 128
EPS = 1e-06
SUB = 16


def dot(a, b):
    return jnp.dot(a, b, preferred_element_type=F32)


def dot_nt(a, b):
    return lax.dot_general(a, b, (((1,), (1,)), ((), ())), preferred_element_type=F32)


def split2(x):
    high = x.astype(BF16)
    return high, (x - high.astype(F32)).astype(BF16)


def lanes(*parts):
    return jnp.concatenate(parts, axis=1)


def rows(*parts):
    return jnp.concatenate(parts, axis=0)


def square_mm(a_parts, b_parts):
    b_both = lanes(*b_parts)
    both = dot(lanes(*a_parts), rows(b_both, b_both))
    return both[:, :N] + both[:, N:]


def wide_mm(a_parts, b_high, b_low):
    return dot(lanes(*a_parts), rows(b_high, b_high)) + dot(a_parts[0], b_low)


def compose(later, earlier):
    high, low = split2(earlier)
    out = wide_mm(split2(later[:, :N]), high, low)
    return out + lanes(jnp.zeros((N, N), F32), later[:, N:])


def iotas():
    return lax.broadcasted_iota(jnp.int32, (N, N), 0), lax.broadcasted_iota(jnp.int32, (N, N), 1)


def terms_kernel(core_ref, kv_ref, map_ref, off_ref, send_ref, *rest):
    outs, (en_ref, grow_ref, wu_hi_ref, wu_lo_ref, node_ref), sems = rest[:5], rest[5:10], rest[10]
    blocks = kv_ref.shape[0]
    copies = []

    def save(which, first=0, count=blocks):
        part = pl.ds(first, count)
        copies.append(
            pltpu.make_async_copy(rest[5 + which].at[part], outs[which].at[part], sems.at[len(copies)])
        )
        copies[-1].start()

    r, c = iotas()
    one = lambda cond: cond.astype(F32).astype(BF16)
    lower = one(r >= c)
    eye16 = one(r == c)
    eye = (r == c).astype(F32)
    inclusive = r >= c
    picks = lanes(one(r > c), jnp.ones((N, N), BF16))
    picks = rows(picks, picks, picks)
    lane16 = lax.broadcasted_iota(jnp.int32, (SUB, N), 1)
    row16 = lax.broadcasted_iota(jnp.int32, (SUB, N), 0)
    start16 = (row16 == lane16 % SUB).astype(F32)
    base16 = lane16 // SUB * SUB
    merge_masks = [one((r // m == c // m + 1) & (c // m % 2 == 0)) for m in (16, 32, 64)]
    group = range(blocks)

    keys = [kv_ref[b, :N, :N] for b in group]
    kk = [dot_nt(k, k) for k in keys]
    aux = [kv_ref[b, N : N + 8, :] for b in group]

    def sums(a):
        left = [rows(lower * a[i : i + 1, :N], eye16 * a[i : i + 1, N:]) for i in range(3)]
        return dot(lanes(*left), picks)

    summed = [sums(a) for a in aux]
    fade = [jnp.exp(s[:N, :N]) for s in summed]
    cum = [s[:N, N:] for s in summed]
    beta_low = [s[N:, :N] for s in summed]
    beta_row = []
    cum_row = []
    for b in group:
        a = aux[b][:8].astype(F32)
        beta_row.append(a[0:1, N:] + a[1:2, N:] + a[2:3, N:])
        cum_row.append(jnp.sum(eye * cum[b], axis=0, keepdims=True))
    diag = [eye * x for x in kk]
    nk_row = [lax.rsqrt(jnp.sum(d, axis=0, keepdims=True) + EPS) for d in diag]
    nk_col = [lax.rsqrt(jnp.sum(d, axis=1, keepdims=True) + EPS) for d in diag]
    low = []
    for b in group:
        fade_n = fade[b] * nk_row[b]
        en_ref[b] = jnp.where(inclusive, fade_n, 0.0)
        low.append(beta_low[b] * fade_n * (nk_col[b] * kk[b]))
        grow_ref[b] = jnp.exp(cum[b])
    save(0)
    save(1)
    inv = []
    for b in group:
        small = sum(
            jnp.where(lane16 // SUB == s, low[b][SUB * s : SUB * (s + 1)], 0.0) for s in range(N // SUB)
        )
        x = start16
        for j in range(SUB - 1):
            col = jnp.take_along_axis(small, base16 + j, axis=1)
            x = x - col * x[j : j + 1, :]
        inv.append(rows(*[jnp.where(lane16 // SUB == s, x, 0.0) for s in range(N // SUB)]))
    low_parts = [split2(x) for x in low]
    for mask in merge_masks:
        parts = [split2(x) for x in inv]
        left = [square_mm(parts[b], [p * mask for p in low_parts[b]]) for b in group]
        left = [split2(x) for x in left]
        inv = [inv[b] - square_mm(left[b], parts[b]) for b in group]
    pairs = []
    for b in group:
        grow_row = jnp.exp(cum_row[b])
        for_u = inv[b] * beta_row[b]
        for_w = for_u * (grow_row * nk_row[b])
        value = kv_ref[b, :N, N:]
        w = dot(lanes(*split2(for_w)), rows(keys[b], keys[b]))
        u = dot(lanes(*split2(for_u)), rows(value, value))
        wu = lanes(w, u)
        wu_hi_ref[b], wu_lo_ref[b] = split2(wu)
        total = cum[b][N - 1 : N, :]
        tail = jnp.exp(total - cum[b]) * nk_col[b]
        high, lo = split2(wu * lanes(tail, tail))
        key_t = keys[b].T
        out = dot(lanes(key_t, key_t), rows(high, lo))
        pair = lanes(eye * jnp.exp(total) - out[:, :N], out[:, N:])
        node_ref[b] = pair
        pairs.append(pair)
    save(2)
    save(3)
    save(4)
    spot = blocks
    while len(pairs) > 2:
        pairs = [compose(pairs[i + 1], pairs[i]) for i in range(0, len(pairs), 2)]
        for i, pair in enumerate(pairs):
            node_ref[spot + i] = pair
        save(4, spot, len(pairs))
        spot += len(pairs)
    total = compose(pairs[1], pairs[0])
    map_ref[...] = total[:, :N]
    off_ref[...] = total[:, N:]
    send_ref[...] = jnp.where(core_ref[0] == 0, total[:, N:], total[:, :N])
    for copy in copies:
        copy.wait()


def reach_kernel(kv_ref, q_ref, *rest):
    sources, (r0_ref, hi_ref, lo_ref) = rest[:5], rest[5:8]
    buffers, sems = rest[8:13], rest[13]
    blocks = kv_ref.shape[0]
    copies = [
        pltpu.make_async_copy(sources[i], buffers[i], sems.at[i]) for i in range(len(sources))
    ]
    for copy in copies:
        copy.start()
    en_ref, wu_hi_ref, wu_lo_ref, grow_ref, node_ref = buffers
    copies[0].wait()
    mixing = [
        split2(en_ref[b] * dot_nt(q_ref[b, :, :N], kv_ref[b, :N, :N])) for b in range(blocks)
    ]
    copies[1].wait()
    copies[2].wait()
    mixed = [wide_mm(mixing[b], wu_hi_ref[b], wu_lo_ref[b]) for b in range(blocks)]
    copies[3].wait()
    copies[4].wait()
    carried = {}
    base, width = {1: 0}, 1
    while width * 2 < blocks:
        base[width * 2] = base[width] + blocks // width
        width *= 2
    step = blocks // 2
    while step:
        for b in range(step, blocks, 2 * step):
            node = node_ref[base[step] + (b - step) // step]
            carried[b] = compose(node, carried[b - step]) if b > step else node
        step //= 2
    for b in range(blocks):
        q = q_ref[b, :, :N]
        q32 = q.astype(F32)
        scale = lax.rsqrt(jnp.sum(q32 * q32, axis=1, keepdims=True) + EPS) * N**-0.5
        reach = grow_ref[b] * q32 - mixed[b][:, :N]
        local = mixed[b][:, N:]
        if b:
            high, low = split2(carried[b])
            out = wide_mm(split2(reach), high, low)
            reach, local = out[:, :N], local + out[:, N:]
        r0_ref[b] = local * scale
        hi_ref[b], lo_ref[b] = split2(reach * scale)


def advance(left, right, extra):
    return square_mm(split2(left), split2(right)) + extra


def pair_kernel(core_ref, map_ref, off_ref, got_ref, out_ref):
    first = core_ref[0] == 0
    own = map_ref[...]
    got = got_ref[...]
    left = jnp.where(first, got, own)
    right = jnp.where(first, own, got)
    out_ref[...] = advance(left, right, jnp.where(first, 0.0, off_ref[...]))


def join_kernel(core_ref, near_ref, map_ref, far_ref, out_ref):
    first = core_ref[0] == 0
    near = near_ref[...]
    left = jnp.where(first, near, map_ref[...])
    out_ref[...] = advance(left, far_ref[...], jnp.where(first, 0.0, near))


def finish_kernel(core_ref, r0_ref, hi_ref, lo_ref, own_ref, swap_ref, far0_ref, far1_ref, map_ref, off_ref, gate_ref, gain_ref, out_ref):
    first = core_ref[0] == 0
    own = own_ref[...]
    swap = swap_ref[...]
    state = advance(
        jnp.where(first, own, swap), far0_ref[...] + far1_ref[...], jnp.where(first, swap, own)
    )
    state = jnp.where(first, state, advance(map_ref[...], state, off_ref[...]))
    y_both = lanes(*split2(state))
    y_both = rows(y_both, y_both)
    for b in range(r0_ref.shape[0]):
        both = dot(lanes(hi_ref[b], lo_ref[b]), y_both)
        res = r0_ref[b] + both[:, :N] + both[:, N:]
        norm = lax.rsqrt(jnp.mean(res * res, axis=1, keepdims=True) + EPS)
        gate = gate_ref[b, :, N:].astype(F32)
        silu = gate / (1.0 + jnp.exp(-gate))
        out_ref[b] = (res * norm * gain_ref[...] * silu).astype(BF16)


def call(kernel, out_shape, inputs, core=None, remote=(), spill=(), sems=0):
    vmem = pl.BlockSpec(memory_space=pltpu.VMEM)
    hbm = pl.BlockSpec(memory_space=pltpu.HBM)
    specs = [vmem] * len(inputs) + [hbm] * len(remote)
    inputs = [*inputs, *(pltpu.with_memory_space_constraint(a, pltpu.HBM) for a in remote)]
    if core is not None:
        specs = [pl.BlockSpec(memory_space=pltpu.SMEM)] + specs
        inputs = [core, *inputs]
    return pl.pallas_call(
        kernel,
        out_shape=[*out_shape, *(pltpu.HBM(o.shape, o.dtype) for o in spill)],
        in_specs=specs,
        out_specs=[vmem] * len(out_shape) + [hbm] * len(spill),
        scratch_shapes=[pltpu.VMEM(o.shape, o.dtype) for o in (*remote, *spill)]
        + ([pltpu.SemaphoreType.DMA((sems,))] if sems else []),
        compiler_params=pltpu.CompilerParams(vmem_limit_bytes=40 * 2**20),
    )(*inputs)


def near(*arrays):
    return [pltpu.with_memory_space_constraint(a, pltpu.VMEM) for a in arrays]


def kept(*dims, dtype=F32):
    return pltpu.VMEM(dims, dtype)


def shape(*dims, dtype=F32):
    return jax.ShapeDtypeStruct(dims, dtype)


def parts3(x):
    high = lax.reduce_precision(x, 8, 7)
    rest = x - high
    mid = lax.reduce_precision(rest, 8, 7)
    return [p.astype(BF16) for p in (high, mid, rest - mid)]


def by_head(array):
    return jnp.transpose(array, (1, 0, 2))


def to_heads(array):
    return lax.all_to_all(array, "head", split_axis=0, concat_axis=0, tiled=True)


def layer(queries, keys, values, beta, log_decay, out_gate, norm_gain):
    z = lax.axis_size("z")
    decay_parts = parts3(jnp.transpose(log_decay))
    beta_parts = parts3(jnp.transpose(beta))
    aux = jnp.concatenate(
        [jnp.stack(decay_parts, axis=1), jnp.stack(beta_parts, axis=1)], axis=2
    )
    aux = jnp.pad(aux, ((0, 0), (0, 5), (0, 0)))
    kv = jnp.concatenate([by_head(keys), by_head(values)], axis=2)
    kv = to_heads(jnp.concatenate([kv, aux], axis=1))
    qg = jnp.concatenate([by_head(queries), by_head(out_gate)], axis=2)
    blocks = kv.shape[0]
    cube = shape(blocks, N, N)
    square = kept(N, N)
    wide16 = shape(blocks, N, 2 * N, dtype=BF16)
    core = lax.axis_index("c").astype(jnp.int32).reshape(1)
    kv, qg = lax.optimization_barrier((kv, qg))
    own_map, own_off, send, en, grow, wu_hi, wu_lo, nodes = call(
        terms_kernel,
        [square] * 3,
        near(kv),
        core,
        spill=[cube, cube, wide16, wide16, shape(2 * blocks - 2, N, 2 * N)],
        sems=8,
    )
    swap = [(0, 1), (1, 0)]
    got = lax.ppermute(send, "c", swap)
    chip = call(pair_kernel, [square], near(own_map, own_off, got), core)[0]

    def up(x, d):
        return lax.ppermute(x, "z", [(i, i + d) for i in range(z - d)])

    def cross(x, d, *routes):
        pairs = [
            (2 * i + source, 2 * (i + d) + target)
            for i in range(z - d)
            for source, target in zip(routes[::2], routes[1::2])
        ]
        return lax.ppermute(x, ("z", "c"), pairs)

    def join(one, maps, far):
        return call(join_kernel, [square], near(one, maps, far), core)[0]

    window, span = chip, 1
    while span * 2 < z:
        far = up(window, span)
        maps = lax.ppermute(window, "c", [(0, 1)])
        if span * 4 >= z:
            qg, maps = lax.optimization_barrier((qg, maps))
            qg = to_heads(qg)
        window = join(window, maps, far)
        span *= 2
    far0 = cross(window, span + 1, 1, 0)
    far1 = cross(window, span + 1, 1, 1)
    own = up(window, 1)
    other = cross(window, 1, 0, 1, 1, 0)
    own_map, own = lax.optimization_barrier((own_map, own))
    first_map = lax.ppermute(own_map, "c", [(0, 1)])
    half = kept(blocks, N, N, dtype=BF16)
    r0, r1_hi, r1_lo = call(
        reach_kernel,
        [kept(blocks, N, N), half, half],
        near(kv, qg),
        remote=[en, wu_hi, wu_lo, grow, nodes],
        sems=5,
    )
    (out,) = call(
        finish_kernel,
        [shape(blocks, N, N, dtype=BF16)],
        near(r0, r1_hi, r1_lo, own, other, far0, far1, first_map, got)
        + [qg, norm_gain.reshape(1, N)],
        core,
    )
    return out.reshape(blocks * N, 1, N)


def solution(mesh):
    finer = Mesh(mesh.devices.reshape(-1, 2, mesh.shape["head"]), ("z", "c", "head"))
    tokens = ("z", "c", "head")
    in_specs = (
        P(tokens, None, None),
        P(tokens, None, None),
        P(tokens, None, None),
        P(tokens, None),
        P(tokens, None),
        P(tokens, None, None),
        P(),
    )
    out_specs = P(("z", "c"), "head", None)
    return jax.shard_map(layer, mesh=finer, in_specs=in_specs, out_specs=out_specs, check_vma=False)
```

```python
import jax
import jax.numpy as jnp
from jax import lax
from jax.experimental import pallas as pl
from jax.experimental.pallas import tpu as pltpu
from jax.sharding import Mesh
from jax.sharding import PartitionSpec as P


F32 = jnp.float32
BF16 = jnp.bfloat16
N = 128
EPS = 1e-06
SUB = 16


def dot(a, b):
    return jnp.dot(a, b, preferred_element_type=F32)


def dot_nt(a, b):
    return lax.dot_general(a, b, (((1,), (1,)), ((), ())), preferred_element_type=F32)


def split2(x):
    high = x.astype(BF16)
    return high, (x - high.astype(F32)).astype(BF16)


def lanes(*parts):
    return jnp.concatenate(parts, axis=1)


def rows(*parts):
    return jnp.concatenate(parts, axis=0)


def square_mm(a_parts, b_parts):
    b_both = lanes(*b_parts)
    both = dot(lanes(*a_parts), rows(b_both, b_both))
    return both[:, :N] + both[:, N:]


def wide_mm(a_parts, b_high, b_low):
    return dot(lanes(*a_parts), rows(b_high, b_high)) + dot(a_parts[0], b_low)


def compose(later, earlier):
    high, low = split2(earlier)
    out = wide_mm(split2(later[:, :N]), high, low)
    return out + lanes(jnp.zeros((N, N), F32), later[:, N:])


def iotas():
    return lax.broadcasted_iota(jnp.int32, (N, N), 0), lax.broadcasted_iota(jnp.int32, (N, N), 1)


def pack_kernel(k_ref, v_ref, beta_ref, decay_ref, out_ref):
    heads, tokens = out_ref.shape[0], k_ref.shape[0] // out_ref.shape[0]
    span = N * 2 // heads
    shape2 = (2 * N, 2 * N)
    r = lax.broadcasted_iota(jnp.int32, shape2, 0)
    c = lax.broadcasted_iota(jnp.int32, shape2, 1)
    order = (c == r % span * heads + r // span).astype(F32).astype(BF16)
    for i in range(tokens // span):
        part = pl.ds(2 * N * i, 2 * N)
        moved = dot(order, lanes(k_ref[part, :], v_ref[part, :])).astype(BF16)
        for h in range(heads):
            out_ref[h, span * i : span * (i + 1), :] = moved[span * h : span * (h + 1), :]
    both = lanes(decay_ref[...].T, beta_ref[...].T)
    high = both.astype(BF16).astype(F32)
    low = both - high
    row = lax.broadcasted_iota(jnp.int32, (8, 2 * N), 0)
    for h in range(heads):
        aux = jnp.where(row == 0, high[h : h + 1, :], jnp.where(row == 1, low[h : h + 1, :], 0.0))
        out_ref[h, tokens : tokens + 8, :] = aux.astype(BF16)


def terms_kernel(kv_ref, total_ref, *rest):
    outs, (en_ref, wu_hi_ref, wu_lo_ref, grow_ref, node_ref), sems = rest[:5], rest[5:10], rest[10]
    blocks = kv_ref.shape[0]
    copies = []

    def save(which, first=0, count=blocks):
        part = pl.ds(first, count)
        copies.append(
            pltpu.make_async_copy(rest[5 + which].at[part], outs[which].at[part], sems.at[len(copies)])
        )
        copies[-1].start()

    r, c = iotas()
    one = lambda cond: cond.astype(F32).astype(BF16)
    lower = one(r >= c)
    eye = (r == c).astype(F32)
    inclusive = r >= c
    strict = r > c
    picks = lanes(one(strict), jnp.ones((N, N), BF16))
    picks = rows(picks, picks)
    lane16 = lax.broadcasted_iota(jnp.int32, (SUB, N), 1)
    row16 = lax.broadcasted_iota(jnp.int32, (SUB, N), 0)
    start16 = (row16 == lane16 % SUB).astype(F32)
    base16 = lane16 // SUB * SUB
    merge_masks = [one((r // m == c // m + 1) & (c // m % 2 == 0)) for m in (16, 32, 64)]
    group = range(blocks)

    keys = [kv_ref[b, :N, :N] for b in group]
    kk = [dot_nt(k, k) for k in keys]
    aux = [kv_ref[b, N : N + 8, :] for b in group]
    summed = [dot(lanes(lower * a[0:1, :N], lower * a[1:2, :N]), picks) for a in aux]
    cum = [s[:, N:] for s in summed]
    beta_row = []
    grow_row = []
    nk_row = []
    nk_col = []
    low = []
    for b in group:
        a = aux[b].astype(F32)
        beta_row.append(a[0:1, N:] + a[1:2, N:])
        grow_row.append(jnp.exp(jnp.sum(eye * cum[b], axis=0, keepdims=True)))
        diag = eye * kk[b]
        nk_row.append(lax.rsqrt(jnp.sum(diag, axis=0, keepdims=True) + EPS))
        nk_col.append(lax.rsqrt(jnp.sum(diag, axis=1, keepdims=True) + EPS))
        beta_col = jnp.sum(eye * beta_row[b], axis=1, keepdims=True)
        fade_n = jnp.exp(summed[b][:, :N]) * nk_row[b]
        en_ref[b] = jnp.where(inclusive, fade_n, 0.0)
        low.append(jnp.where(strict, fade_n * (kk[b] * (beta_col * nk_col[b])), 0.0))
        grow_ref[b] = jnp.broadcast_to(grow_row[b], (8, N))
    save(0)
    save(3)
    inv = []
    for b in group:
        small = sum(
            jnp.where(lane16 // SUB == s, low[b][SUB * s : SUB * (s + 1)], 0.0) for s in range(N // SUB)
        )
        x = start16
        for j in range(SUB - 1):
            col = jnp.take_along_axis(small, base16 + j, axis=1)
            x = x - col * x[j : j + 1, :]
        inv.append(rows(*[jnp.where(lane16 // SUB == s, x, 0.0) for s in range(N // SUB)]))
    low_parts = [split2(x) for x in low]
    for mask in merge_masks:
        parts = [split2(x) for x in inv]
        left = [square_mm(parts[b], [p * mask for p in low_parts[b]]) for b in group]
        left = [split2(x) for x in left]
        inv = [inv[b] - square_mm(left[b], parts[b]) for b in group]
    for_u = [inv[b] * beta_row[b] for b in group]
    for_w = [split2(for_u[b] * (grow_row[b] * nk_row[b])) for b in group]
    for_u = [split2(x) for x in for_u]
    w = [dot(lanes(*for_w[b]), rows(keys[b], keys[b])) for b in group]
    values = [kv_ref[b, :N, N:] for b in group]
    u = [dot(lanes(*for_u[b]), rows(values[b], values[b])) for b in group]
    wu = [lanes(w[b], u[b]) for b in group]
    for b in group:
        wu_hi_ref[b], wu_lo_ref[b] = split2(wu[b])
    save(1)
    save(2)
    last = [x[N - 1 : N, :] for x in cum]
    tail = [jnp.exp(last[b] - cum[b]) * nk_col[b] for b in group]
    faded = [split2(wu[b] * lanes(tail[b], tail[b])) for b in group]
    key_t = [k.T for k in keys]
    out = [dot(lanes(key_t[b], key_t[b]), rows(*faded[b])) for b in group]
    pairs = [lanes(eye * jnp.exp(last[b]) - out[b][:, :N], out[b][:, N:]) for b in group]
    spot = 0
    while len(pairs) > 1:
        for i in range(0, len(pairs), 2):
            node_ref[spot + i // 2] = pairs[i]
        save(4, spot, len(pairs) // 2)
        spot += len(pairs) // 2
        pairs = [compose(pairs[i + 1], pairs[i]) for i in range(0, len(pairs), 2)]
    total_ref[...] = pairs[0]
    for copy in copies:
        copy.wait()


def reach_kernel(kv_ref, qg_ref, gain_ref, *rest):
    sources, (r0_ref, hi_ref, lo_ref, gate_ref) = rest[:5], rest[5:9]
    buffers, sems = rest[9:14], rest[14]
    blocks = kv_ref.shape[0]
    copies = [
        pltpu.make_async_copy(sources[i], buffers[i], sems.at[i]) for i in range(len(sources))
    ]
    for copy in copies:
        copy.start()
    en_ref, wu_hi_ref, wu_lo_ref, grow_ref, node_ref = buffers
    r, c = iotas()
    eye = (r == c).astype(F32)
    for b in range(blocks):
        gate = qg_ref[b, :, N:].astype(F32)
        gate_ref[b] = gate / (1.0 + jnp.exp(-gate)) * gain_ref[...]
    copies[0].wait()
    mixing = [
        split2(en_ref[b] * dot_nt(qg_ref[b, :, :N], kv_ref[b, :N, :N])) for b in range(blocks)
    ]
    copies[1].wait()
    copies[2].wait()
    mixed = [wide_mm(mixing[b], wu_hi_ref[b], wu_lo_ref[b]) for b in range(blocks)]
    copies[3].wait()
    copies[4].wait()
    carried = {}
    base, width = {1: 0}, 1
    while width * 2 < blocks:
        base[width * 2] = base[width] + blocks // width // 2
        width *= 2
    step = blocks // 2
    while step:
        for b in range(step, blocks, 2 * step):
            node = node_ref[base[step] + (b - step) // step // 2]
            carried[b] = compose(node, carried[b - step]) if b > step else node
        step //= 2
    for b in range(blocks):
        q32 = qg_ref[b, :, :N].astype(F32)
        scale = lax.rsqrt(jnp.sum(q32 * q32, axis=1, keepdims=True) + EPS) * N**-0.5
        grow_col = jnp.sum(eye * grow_ref[b, 0:1, :], axis=1, keepdims=True)
        reach = grow_col * q32 - mixed[b][:, :N]
        local = mixed[b][:, N:]
        if b:
            high, low = split2(carried[b])
            out = wide_mm(split2(reach), high, low)
            reach, local = out[:, :N], local + out[:, N:]
        r0_ref[b] = local * scale
        hi_ref[b], lo_ref[b] = split2(reach * scale)


def advance(left, right, extra):
    return square_mm(split2(left), split2(right)) + extra


def pair_kernel(core_ref, own_ref, got_ref, out_ref):
    first = core_ref[0] == 0
    own = own_ref[...]
    got = got_ref[...]
    out_ref[...] = compose(jnp.where(first, got, own), jnp.where(first, own, got))


def join_kernel(core_ref, near_ref, far_ref, out_ref, half_ref):
    out = compose(near_ref[...], far_ref[...])
    out_ref[...] = out
    half_ref[...] = jnp.where(core_ref[0] == 0, out[:, :N], out[:, N:])


def half_kernel(core_ref, near_ref, far_ref, out_ref):
    near = near_ref[...]
    extra = jnp.where(core_ref[0] == 0, 0.0, near[:, N:])
    out_ref[...] = advance(near[:, :N], far_ref[...], extra)


def finish_kernel(core_ref, r0_ref, hi_ref, lo_ref, own_ref, swap_ref, far0_ref, far1_ref, first_ref, gate_ref, out_ref):
    first = core_ref[0] == 0
    own = own_ref[...]
    swap = swap_ref[...]
    state = advance(
        jnp.where(first, own, swap), far0_ref[...] + far1_ref[...], jnp.where(first, swap, own)
    )
    state = jnp.where(first, state, advance(first_ref[:, :N], state, first_ref[:, N:]))
    y_both = lanes(*split2(state))
    y_both = rows(y_both, y_both)
    for b in range(r0_ref.shape[0]):
        both = dot(lanes(hi_ref[b], lo_ref[b]), y_both)
        res = r0_ref[b] + both[:, :N] + both[:, N:]
        norm = lax.rsqrt(jnp.mean(res * res, axis=1, keepdims=True) + EPS)
        out_ref[b] = (res * norm * gate_ref[b]).astype(BF16)


def call(kernel, out_shape, inputs, core=None, remote=(), spill=(), sems=0):
    vmem = pl.BlockSpec(memory_space=pltpu.VMEM)
    hbm = pl.BlockSpec(memory_space=pltpu.HBM)
    specs = [vmem] * len(inputs) + [hbm] * len(remote)
    inputs = [*inputs, *(pltpu.with_memory_space_constraint(a, pltpu.HBM) for a in remote)]
    if core is not None:
        specs = [pl.BlockSpec(memory_space=pltpu.SMEM)] + specs
        inputs = [core, *inputs]
    return pl.pallas_call(
        kernel,
        out_shape=[*out_shape, *(pltpu.HBM(o.shape, o.dtype) for o in spill)],
        in_specs=specs,
        out_specs=[vmem] * len(out_shape) + [hbm] * len(spill),
        scratch_shapes=[pltpu.VMEM(o.shape, o.dtype) for o in (*remote, *spill)]
        + ([pltpu.SemaphoreType.DMA((sems,))] if sems else []),
        compiler_params=pltpu.CompilerParams(vmem_limit_bytes=40 * 2**20),
    )(*inputs)


def near(*arrays):
    return [pltpu.with_memory_space_constraint(a, pltpu.VMEM) for a in arrays]


def kept(*dims, dtype=F32):
    return pltpu.VMEM(dims, dtype)


def shape(*dims, dtype=F32):
    return jax.ShapeDtypeStruct(dims, dtype)


def by_head(array):
    return jnp.transpose(array, (1, 0, 2))


def to_heads(array):
    return lax.all_to_all(array, "head", split_axis=0, concat_axis=0, tiled=True)


def layer(queries, keys, values, beta, log_decay, out_gate, norm_gain):
    tokens, heads, _ = values.shape
    z = lax.axis_size("z")
    flat = lambda array: array.reshape(tokens * heads, N)
    (kv,) = call(
        pack_kernel,
        [kept(heads, tokens + 8, 2 * N, dtype=BF16)],
        [flat(keys), flat(values), beta, log_decay],
    )
    kv = to_heads(kv)
    qg = jnp.concatenate([by_head(queries), by_head(out_gate)], axis=2)
    blocks = kv.shape[0]
    square = kept(N, N)
    wide = kept(N, 2 * N)
    wide16 = shape(blocks, N, 2 * N, dtype=BF16)
    core = lax.axis_index("c").astype(jnp.int32).reshape(1)
    kv, qg = lax.optimization_barrier((kv, qg))
    total, en, wu_hi, wu_lo, grow, nodes = call(
        terms_kernel,
        [wide],
        near(kv),
        spill=[
            shape(blocks, N, N),
            wide16,
            wide16,
            shape(blocks, 8, N),
            shape(blocks - 1, N, 2 * N),
        ],
        sems=8,
    )
    got = lax.ppermute(total, "c", [(0, 1), (1, 0)])
    (window,) = call(pair_kernel, [wide], near(total, got), core)

    def up(x, d):
        return lax.ppermute(x, "z", [(i, i + d) for i in range(z - d)])

    def cross(x, d, *routes):
        pairs = [
            (2 * i + source, 2 * (i + d) + target)
            for i in range(z - d)
            for source, target in zip(routes[::2], routes[1::2])
        ]
        return lax.ppermute(x, ("z", "c"), pairs)

    span = 1
    while span * 4 < z:
        window, half = call(join_kernel, [wide, square], near(window, up(window, span)), core)
        span *= 2
    far = up(half, span)
    qg, half = lax.optimization_barrier((qg, half))
    qg = to_heads(qg)
    (half,) = call(half_kernel, [square], near(window, far), core)
    span *= 2
    own = up(half, 1)
    other = cross(half, 1, 0, 1, 1, 0)
    far0 = cross(half, span + 1, 1, 0)
    far1 = cross(half, span + 1, 1, 1)
    cube = kept(blocks, N, N)
    cube16 = kept(blocks, N, N, dtype=BF16)
    r0, r1_hi, r1_lo, gate = call(
        reach_kernel,
        [cube, cube16, cube16, cube],
        [*near(kv, qg), norm_gain.reshape(1, N)],
        remote=[en, wu_hi, wu_lo, grow, nodes],
        sems=5,
    )
    (out,) = call(
        finish_kernel,
        [shape(blocks, N, N, dtype=BF16)],
        near(r0, r1_hi, r1_lo, own, other, far0, far1, got, gate),
        core,
    )
    return out.reshape(blocks * N, 1, N)


def solution(mesh):
    finer = Mesh(mesh.devices.reshape(-1, 2, mesh.shape["head"]), ("z", "c", "head"))
    tokens = ("z", "c", "head")
    in_specs = (
        P(tokens, None, None),
        P(tokens, None, None),
        P(tokens, None, None),
        P(tokens, None),
        P(tokens, None),
        P(tokens, None, None),
        P(),
    )
    out_specs = P(("z", "c"), "head", None)
    return jax.shard_map(layer, mesh=finer, in_specs=in_specs, out_specs=out_specs, check_vma=False)
```

```python
import jax
import jax.numpy as jnp
from jax import lax
from jax.experimental import pallas as pl
from jax.experimental.pallas import tpu as pltpu
from jax.sharding import Mesh
from jax.sharding import PartitionSpec as P


F32 = jnp.float32
BF16 = jnp.bfloat16
N = 128
EPS = 1e-06
SUB = 16


def dot(a, b):
    return jnp.dot(a, b, preferred_element_type=F32)


def dot_nt(a, b):
    return lax.dot_general(a, b, (((1,), (1,)), ((), ())), preferred_element_type=F32)


def split2(x):
    high = x.astype(BF16)
    return high, (x - high.astype(F32)).astype(BF16)


def lanes(*parts):
    return jnp.concatenate(parts, axis=1)


def rows(*parts):
    return jnp.concatenate(parts, axis=0)


def square_mm(a_parts, b_parts):
    b_both = lanes(*b_parts)
    both = dot(lanes(*a_parts), rows(b_both, b_both))
    return both[:, :N] + both[:, N:]


def wide_mm(a_parts, b_high, b_low):
    return dot(lanes(*a_parts), rows(b_high, b_high)) + dot(a_parts[0], b_low)


def compose(later, earlier):
    high, low = split2(earlier)
    out = wide_mm(split2(later[:, :N]), high, low)
    return out + lanes(jnp.zeros((N, N), F32), later[:, N:])


def iotas():
    return lax.broadcasted_iota(jnp.int32, (N, N), 0), lax.broadcasted_iota(jnp.int32, (N, N), 1)


def pack_kernel(k_hbm, v_hbm, beta_hbm, decay_hbm, out_ref, k_ref, v_ref, beta_ref, decay_ref, sems):
    heads, tokens = out_ref.shape[0], k_ref.shape[0] // out_ref.shape[0]
    span = N * 2 // heads
    quarter = k_ref.shape[0] // 4
    copies = []
    for i in range(4):
        part = pl.ds(quarter * i, quarter)
        for j, (source, target) in enumerate(((k_hbm, k_ref), (v_hbm, v_ref))):
            copies.append(
                pltpu.make_async_copy(source.at[part], target.at[part], sems.at[2 * i + j])
            )
            copies[-1].start()
    for i, (source, target) in enumerate(((beta_hbm, beta_ref), (decay_hbm, decay_ref))):
        copies.append(pltpu.make_async_copy(source, target, sems.at[8 + i]))
        copies[-1].start()
    shape2 = (2 * N, 2 * N)
    r = lax.broadcasted_iota(jnp.int32, shape2, 0)
    c = lax.broadcasted_iota(jnp.int32, shape2, 1)
    order = (c == r % span * heads + r // span).astype(F32).astype(BF16)
    for i in range(tokens // span):
        part = pl.ds(2 * N * i, 2 * N)
        if 2 * N * i % quarter == 0:
            copies[2 * N * i // quarter * 2].wait()
            copies[2 * N * i // quarter * 2 + 1].wait()
        moved = dot(order, lanes(k_ref[part, :], v_ref[part, :])).astype(BF16)
        for h in range(heads):
            out_ref[h, span * i : span * (i + 1), :] = moved[span * h : span * (h + 1), :]
    copies[8].wait()
    copies[9].wait()
    both = lanes(decay_ref[...], beta_ref[...])
    high = both.astype(BF16).astype(F32)
    low = both - high
    row = lax.broadcasted_iota(jnp.int32, (8, 2 * N), 0)
    for h in range(heads):
        aux = jnp.where(row == 0, high[h : h + 1, :], jnp.where(row == 1, low[h : h + 1, :], 0.0))
        out_ref[h, tokens : tokens + 8, :] = aux.astype(BF16)


def terms_kernel(kv_ref, total_ref, *rest):
    outs, (en_ref, wu_hi_ref, wu_lo_ref, grow_ref, node_ref), sems = rest[:5], rest[5:10], rest[10]
    blocks = kv_ref.shape[0]
    copies = []

    def save(which, first=0, count=blocks):
        part = pl.ds(first, count)
        copies.append(
            pltpu.make_async_copy(rest[5 + which].at[part], outs[which].at[part], sems.at[len(copies)])
        )
        copies[-1].start()

    r, c = iotas()
    one = lambda cond: cond.astype(F32).astype(BF16)
    lower = one(r >= c)
    eye = (r == c).astype(F32)
    inclusive = r >= c
    strict = r > c
    picks = lanes(one(strict), jnp.ones((N, N), BF16))
    picks = rows(picks, picks)
    lane16 = lax.broadcasted_iota(jnp.int32, (SUB, N), 1)
    row16 = lax.broadcasted_iota(jnp.int32, (SUB, N), 0)
    start16 = (row16 == lane16 % SUB).astype(F32)
    base16 = lane16 // SUB * SUB
    merge_masks = [one((r // m == c // m + 1) & (c // m % 2 == 0)) for m in (16, 32, 64)]
    group = range(blocks)

    keys = [kv_ref[b, :N, :N] for b in group]
    kk = [dot_nt(k, k) for k in keys]
    aux = [kv_ref[b, N : N + 8, :] for b in group]
    summed = [dot(lanes(lower * a[0:1, :N], lower * a[1:2, :N]), picks) for a in aux]
    cum = [s[:, N:] for s in summed]
    beta_row = []
    grow_row = []
    nk_row = []
    nk_col = []
    low = []
    for b in group:
        a = aux[b].astype(F32)
        beta_row.append(a[0:1, N:] + a[1:2, N:])
        grow_row.append(jnp.exp(jnp.sum(eye * cum[b], axis=0, keepdims=True)))
        diag = eye * kk[b]
        nk_row.append(lax.rsqrt(jnp.sum(diag, axis=0, keepdims=True) + EPS))
        nk_col.append(lax.rsqrt(jnp.sum(diag, axis=1, keepdims=True) + EPS))
        beta_col = jnp.sum(eye * beta_row[b], axis=1, keepdims=True)
        fade_n = jnp.exp(summed[b][:, :N]) * nk_row[b]
        en_ref[b] = jnp.where(inclusive, fade_n, 0.0)
        low.append(jnp.where(strict, fade_n * (kk[b] * (beta_col * nk_col[b])), 0.0))
        grow_ref[b] = jnp.broadcast_to(grow_row[b], (8, N))
    save(0)
    save(3)
    inv = []
    for b in group:
        small = sum(
            jnp.where(lane16 // SUB == s, low[b][SUB * s : SUB * (s + 1)], 0.0) for s in range(N // SUB)
        )
        x = start16
        for j in range(SUB - 1):
            col = jnp.take_along_axis(small, base16 + j, axis=1)
            x = x - col * x[j : j + 1, :]
        inv.append(rows(*[jnp.where(lane16 // SUB == s, x, 0.0) for s in range(N // SUB)]))
    low_parts = [split2(x) for x in low]
    for mask in merge_masks:
        parts = [split2(x) for x in inv]
        left = [square_mm(parts[b], [p * mask for p in low_parts[b]]) for b in group]
        left = [split2(x) for x in left]
        inv = [inv[b] - square_mm(left[b], parts[b]) for b in group]
    for_u = [inv[b] * beta_row[b] for b in group]
    for_w = [split2(for_u[b] * (grow_row[b] * nk_row[b])) for b in group]
    for_u = [split2(x) for x in for_u]
    w = [dot(lanes(*for_w[b]), rows(keys[b], keys[b])) for b in group]
    values = [kv_ref[b, :N, N:] for b in group]
    u = [dot(lanes(*for_u[b]), rows(values[b], values[b])) for b in group]
    wu = [lanes(w[b], u[b]) for b in group]
    for b in group:
        wu_hi_ref[b], wu_lo_ref[b] = split2(wu[b])
    save(1)
    save(2)
    last = [x[N - 1 : N, :] for x in cum]
    tail = [jnp.exp(last[b] - cum[b]) * nk_col[b] for b in group]
    faded = [split2(wu[b] * lanes(tail[b], tail[b])) for b in group]
    key_t = [k.T for k in keys]
    out = [dot(lanes(key_t[b], key_t[b]), rows(*faded[b])) for b in group]
    pairs = [lanes(eye * jnp.exp(last[b]) - out[b][:, :N], out[b][:, N:]) for b in group]
    spot = 0
    while len(pairs) > 1:
        for i in range(0, len(pairs), 2):
            node_ref[spot + i // 2] = pairs[i]
        save(4, spot, len(pairs) // 2)
        spot += len(pairs) // 2
        pairs = [compose(pairs[i + 1], pairs[i]) for i in range(0, len(pairs), 2)]
    total_ref[...] = pairs[0]
    for copy in copies:
        copy.wait()


def reach_kernel(kv_ref, qg_ref, gain_ref, *rest):
    sources, (r0_ref, hi_ref, lo_ref, gate_ref) = rest[:5], rest[5:9]
    buffers, sems = rest[9:14], rest[14]
    blocks = kv_ref.shape[0]
    copies = [
        pltpu.make_async_copy(sources[i], buffers[i], sems.at[i]) for i in range(len(sources))
    ]
    for copy in copies:
        copy.start()
    en_ref, wu_hi_ref, wu_lo_ref, grow_ref, node_ref = buffers
    r, c = iotas()
    eye = (r == c).astype(F32)
    for b in range(blocks):
        gate = qg_ref[b, :, N:].astype(F32)
        gate_ref[b] = gate / (1.0 + jnp.exp(-gate)) * gain_ref[...]
    copies[0].wait()
    mixing = [
        split2(en_ref[b] * dot_nt(qg_ref[b, :, :N], kv_ref[b, :N, :N])) for b in range(blocks)
    ]
    copies[1].wait()
    copies[2].wait()
    mixed = [wide_mm(mixing[b], wu_hi_ref[b], wu_lo_ref[b]) for b in range(blocks)]
    copies[3].wait()
    copies[4].wait()
    carried = {}
    base, width = {1: 0}, 1
    while width * 2 < blocks:
        base[width * 2] = base[width] + blocks // width // 2
        width *= 2
    step = blocks // 2
    while step:
        for b in range(step, blocks, 2 * step):
            node = node_ref[base[step] + (b - step) // step // 2]
            carried[b] = compose(node, carried[b - step]) if b > step else node
        step //= 2
    for b in range(blocks):
        q32 = qg_ref[b, :, :N].astype(F32)
        scale = lax.rsqrt(jnp.sum(q32 * q32, axis=1, keepdims=True) + EPS) * N**-0.5
        grow_col = jnp.sum(eye * grow_ref[b, 0:1, :], axis=1, keepdims=True)
        reach = grow_col * q32 - mixed[b][:, :N]
        local = mixed[b][:, N:]
        if b:
            high, low = split2(carried[b])
            out = wide_mm(split2(reach), high, low)
            reach, local = out[:, :N], local + out[:, N:]
        r0_ref[b] = local * scale
        hi_ref[b], lo_ref[b] = split2(reach * scale)


def advance(left, right, extra):
    return square_mm(split2(left), split2(right)) + extra


def pair_kernel(core_ref, own_ref, got_ref, out_ref):
    first = core_ref[0] == 0
    own = own_ref[:, :N]
    left = jnp.where(first, got_ref[:, :N], own)
    right = jnp.where(first, own, got_ref[:, N:])
    out_ref[...] = advance(left, right, jnp.where(first, 0.0, own_ref[:, N:]))


def join_kernel(core_ref, near_ref, map_ref, far_ref, out_ref):
    first = core_ref[0] == 0
    near = near_ref[...]
    left = jnp.where(first, near, map_ref[...])
    out_ref[...] = advance(left, far_ref[...], jnp.where(first, 0.0, near))


def finish_kernel(core_ref, r0_ref, hi_ref, lo_ref, own_ref, swap_ref, first_ref, gate_ref, *rest):
    *far_refs, out_ref = rest
    first = core_ref[0] == 0
    own = own_ref[...]
    swap = swap_ref[...]
    state = advance(
        jnp.where(first, own, swap), sum(ref[...] for ref in far_refs), jnp.where(first, swap, own)
    )
    state = jnp.where(first, state, advance(first_ref[:, :N], state, first_ref[:, N:]))
    y_both = lanes(*split2(state))
    y_both = rows(y_both, y_both)
    for b in range(r0_ref.shape[0]):
        both = dot(lanes(hi_ref[b], lo_ref[b]), y_both)
        res = r0_ref[b] + both[:, :N] + both[:, N:]
        norm = lax.rsqrt(jnp.mean(res * res, axis=1, keepdims=True) + EPS)
        out_ref[b] = (res * norm * gate_ref[b]).astype(BF16)


def call(kernel, out_shape, inputs, core=None, remote=(), spill=(), sems=0):
    vmem = pl.BlockSpec(memory_space=pltpu.VMEM)
    hbm = pl.BlockSpec(memory_space=pltpu.HBM)
    specs = [vmem] * len(inputs) + [hbm] * len(remote)
    inputs = [*inputs, *(pltpu.with_memory_space_constraint(a, pltpu.HBM) for a in remote)]
    if core is not None:
        specs = [pl.BlockSpec(memory_space=pltpu.SMEM)] + specs
        inputs = [core, *inputs]
    return pl.pallas_call(
        kernel,
        out_shape=[*out_shape, *(pltpu.HBM(o.shape, o.dtype) for o in spill)],
        in_specs=specs,
        out_specs=[vmem] * len(out_shape) + [hbm] * len(spill),
        scratch_shapes=[pltpu.VMEM(o.shape, o.dtype) for o in (*remote, *spill)]
        + ([pltpu.SemaphoreType.DMA((sems,))] if sems else []),
        compiler_params=pltpu.CompilerParams(vmem_limit_bytes=40 * 2**20),
    )(*inputs)


def near(*arrays):
    return [pltpu.with_memory_space_constraint(a, pltpu.VMEM) for a in arrays]


def kept(*dims, dtype=F32):
    return pltpu.VMEM(dims, dtype)


def shape(*dims, dtype=F32):
    return jax.ShapeDtypeStruct(dims, dtype)


def by_head(array):
    return jnp.transpose(array, (1, 0, 2))


def to_heads(array):
    return lax.all_to_all(array, "head", split_axis=0, concat_axis=0, tiled=True)


def layer(queries, keys, values, beta, log_decay, out_gate, norm_gain):
    tokens, heads, _ = values.shape
    z = lax.axis_size("z")
    flat = lambda array: array.reshape(tokens * heads, N)
    (kv,) = call(
        pack_kernel,
        [kept(heads, tokens + 8, 2 * N, dtype=BF16)],
        [],
        remote=[flat(keys), flat(values), beta.T, log_decay.T],
        sems=10,
    )
    kv = to_heads(kv)
    qg = jnp.concatenate([by_head(queries), by_head(out_gate)], axis=2)
    blocks = kv.shape[0]
    square = kept(N, N)
    wide = kept(N, 2 * N)
    wide16 = shape(blocks, N, 2 * N, dtype=BF16)
    core = lax.axis_index("c").astype(jnp.int32).reshape(1)
    kv, qg = lax.optimization_barrier((kv, qg))
    total, en, wu_hi, wu_lo, grow, nodes = call(
        terms_kernel,
        [wide],
        near(kv),
        spill=[
            shape(blocks, N, N),
            wide16,
            wide16,
            shape(blocks, 8, N),
            shape(blocks - 1, N, 2 * N),
        ],
        sems=8,
    )
    got = lax.ppermute(total, "c", [(0, 1), (1, 0)])
    (window,) = call(pair_kernel, [square], near(total, got), core)

    def up(x, d):
        return lax.ppermute(x, "z", [(i, i + d) for i in range(z - d)])

    def cross(x, d, sources, *routes):
        pairs = [
            (2 * i + source, 2 * (i + d) + target)
            for i in sources
            for source, target in zip(routes[::2], routes[1::2])
        ]
        return lax.ppermute(x, ("z", "c"), pairs)

    span, reach_back = 1, z // 2 + 1
    while span * 2 < z:
        far = up(window, span)
        maps = lax.ppermute(window, "c", [(0, 1)])
        if span * 4 >= z:
            done = range(min(span, z - reach_back))
            fars = [cross(window, reach_back, done, 1, target) for target in (0, 1)]
        elif span * 8 >= z:
            qg, window = lax.optimization_barrier((qg, window))
            qg = to_heads(qg)
        (window,) = call(join_kernel, [square], near(window, maps, far), core)
        span *= 2
    left = range(len(done), z - reach_back)
    fars += [cross(window, reach_back, left, 1, target) for target in (0, 1)]
    own = up(window, 1)
    other = cross(window, 1, range(z - 1), 0, 1, 1, 0)
    cube = kept(blocks, N, N)
    cube16 = kept(blocks, N, N, dtype=BF16)
    r0, r1_hi, r1_lo, gate = call(
        reach_kernel,
        [cube, cube16, cube16, cube],
        [*near(kv, qg), norm_gain.reshape(1, N)],
        remote=[en, wu_hi, wu_lo, grow, nodes],
        sems=5,
    )
    (out,) = call(
        finish_kernel,
        [shape(blocks, N, N, dtype=BF16)],
        near(r0, r1_hi, r1_lo, own, other, got, gate, *fars),
        core,
    )
    return out.reshape(blocks * N, 1, N)


def solution(mesh):
    finer = Mesh(mesh.devices.reshape(-1, 2, mesh.shape["head"]), ("z", "c", "head"))
    tokens = ("z", "c", "head")
    in_specs = (
        P(tokens, None, None),
        P(tokens, None, None),
        P(tokens, None, None),
        P(tokens, None),
        P(tokens, None),
        P(tokens, None, None),
        P(),
    )
    out_specs = P(("z", "c"), "head", None)
    return jax.shard_map(layer, mesh=finer, in_specs=in_specs, out_specs=out_specs, check_vma=False)
```

```python
import jax
import jax.numpy as jnp
from jax import lax
from jax.experimental import pallas as pl
from jax.experimental.pallas import tpu as pltpu
from jax.sharding import Mesh
from jax.sharding import PartitionSpec as P


F32 = jnp.float32
BF16 = jnp.bfloat16
N = 128
EPS = 1e-06
SUB = 16


def dot(a, b):
    return jnp.dot(a, b, preferred_element_type=F32)


def dot_nt(a, b):
    return lax.dot_general(a, b, (((1,), (1,)), ((), ())), preferred_element_type=F32)


def split2(x):
    high = x.astype(BF16)
    return high, (x - high.astype(F32)).astype(BF16)


def lanes(*parts):
    return jnp.concatenate(parts, axis=1)


def rows(*parts):
    return jnp.concatenate(parts, axis=0)


def square_mm(a_parts, b_parts):
    b_both = lanes(*b_parts)
    both = dot(lanes(*a_parts), rows(b_both, b_both))
    return both[:, :N] + both[:, N:]


def wide_mm(a_parts, b_high, b_low):
    return dot(lanes(*a_parts), rows(b_high, b_high)) + dot(a_parts[0], b_low)


def compose(later, earlier):
    high, low = split2(earlier)
    out = wide_mm(split2(later[:, :N]), high, low)
    return out + lanes(jnp.zeros((N, N), F32), later[:, N:])


def iotas():
    return lax.broadcasted_iota(jnp.int32, (N, N), 0), lax.broadcasted_iota(jnp.int32, (N, N), 1)


def pack_kernel(k_hbm, v_hbm, beta_hbm, decay_hbm, out_hbm, k_ref, v_ref, beta_ref, decay_ref, out_ref, sems):
    heads, tokens = out_ref.shape[0], k_ref.shape[0] // out_ref.shape[0]
    span = N * 2 // heads
    quarter = k_ref.shape[0] // 4
    copies = []
    for i in range(4):
        part = pl.ds(quarter * i, quarter)
        for j, (source, target) in enumerate(((k_hbm, k_ref), (v_hbm, v_ref))):
            copies.append(
                pltpu.make_async_copy(source.at[part], target.at[part], sems.at[2 * i + j])
            )
            copies[-1].start()
    for i, (source, target) in enumerate(((beta_hbm, beta_ref), (decay_hbm, decay_ref))):
        copies.append(pltpu.make_async_copy(source, target, sems.at[8 + i]))
        copies[-1].start()

    def send(first, count):
        part = pl.ds(first, count)
        copies.append(
            pltpu.make_async_copy(
                out_ref.at[:, part, :], out_hbm.at[:, part, :], sems.at[len(copies)]
            )
        )
        copies[-1].start()

    shape2 = (2 * N, 2 * N)
    r = lax.broadcasted_iota(jnp.int32, shape2, 0)
    c = lax.broadcasted_iota(jnp.int32, shape2, 1)
    order = (c == r % span * heads + r // span).astype(F32).astype(BF16)
    for i in range(tokens // span):
        part = pl.ds(2 * N * i, 2 * N)
        if 2 * N * i % quarter == 0:
            copies[2 * N * i // quarter * 2].wait()
            copies[2 * N * i // quarter * 2 + 1].wait()
        moved = dot(order, lanes(k_ref[part, :], v_ref[part, :])).astype(BF16)
        for h in range(heads):
            out_ref[h, span * i : span * (i + 1), :] = moved[span * h : span * (h + 1), :]
        if 2 * N * (i + 1) % quarter == 0:
            send(span * (i + 1) - tokens // 4, tokens // 4)
    copies[8].wait()
    copies[9].wait()
    both = lanes(decay_ref[...], beta_ref[...])
    high = both.astype(BF16).astype(F32)
    low = both - high
    row = lax.broadcasted_iota(jnp.int32, (8, 2 * N), 0)
    for h in range(heads):
        aux = jnp.where(row == 0, high[h : h + 1, :], jnp.where(row == 1, low[h : h + 1, :], 0.0))
        out_ref[h, tokens : tokens + 8, :] = aux.astype(BF16)
    send(tokens, 8)
    for copy in copies[10:]:
        copy.wait()


def terms_kernel(kv_ref, total_ref, *rest):
    outs, (en_ref, wu_hi_ref, wu_lo_ref, grow_ref, node_ref), sems = rest[:5], rest[5:10], rest[10]
    blocks = kv_ref.shape[0]
    copies = []

    def save(which, first=0, count=blocks):
        part = pl.ds(first, count)
        copies.append(
            pltpu.make_async_copy(rest[5 + which].at[part], outs[which].at[part], sems.at[len(copies)])
        )
        copies[-1].start()

    r, c = iotas()
    one = lambda cond: cond.astype(F32).astype(BF16)
    lower = one(r >= c)
    eye = (r == c).astype(F32)
    inclusive = r >= c
    strict = r > c
    picks = lanes(one(strict), jnp.ones((N, N), BF16))
    picks = rows(picks, picks)
    lane16 = lax.broadcasted_iota(jnp.int32, (SUB, N), 1)
    row16 = lax.broadcasted_iota(jnp.int32, (SUB, N), 0)
    start16 = (row16 == lane16 % SUB).astype(F32)
    base16 = lane16 // SUB * SUB
    merge_masks = [one((r // m == c // m + 1) & (c // m % 2 == 0)) for m in (16, 32, 64)]
    group = range(blocks)

    keys = [kv_ref[b, :N, :N] for b in group]
    kk = [dot_nt(k, k) for k in keys]
    aux = [kv_ref[b, N : N + 8, :] for b in group]
    summed = [dot(lanes(lower * a[0:1, :N], lower * a[1:2, :N]), picks) for a in aux]
    cum = [s[:, N:] for s in summed]
    beta_row = []
    grow_row = []
    nk_row = []
    nk_col = []
    low = []
    for b in group:
        a = aux[b].astype(F32)
        beta_row.append(a[0:1, N:] + a[1:2, N:])
        grow_row.append(jnp.exp(jnp.sum(eye * cum[b], axis=0, keepdims=True)))
        diag = eye * kk[b]
        nk_row.append(lax.rsqrt(jnp.sum(diag, axis=0, keepdims=True) + EPS))
        nk_col.append(lax.rsqrt(jnp.sum(diag, axis=1, keepdims=True) + EPS))
        beta_col = jnp.sum(eye * beta_row[b], axis=1, keepdims=True)
        fade_n = jnp.exp(summed[b][:, :N]) * nk_row[b]
        en_ref[b] = jnp.where(inclusive, fade_n, 0.0)
        low.append(jnp.where(strict, fade_n * (kk[b] * (beta_col * nk_col[b])), 0.0))
        grow_ref[b] = jnp.broadcast_to(grow_row[b], (8, N))
    save(0)
    save(3)
    inv = []
    for b in group:
        small = sum(
            jnp.where(lane16 // SUB == s, low[b][SUB * s : SUB * (s + 1)], 0.0) for s in range(N // SUB)
        )
        x = start16
        for j in range(SUB - 1):
            col = jnp.take_along_axis(small, base16 + j, axis=1)
            x = x - col * x[j : j + 1, :]
        inv.append(rows(*[jnp.where(lane16 // SUB == s, x, 0.0) for s in range(N // SUB)]))
    low_parts = [split2(x) for x in low]
    for mask in merge_masks:
        parts = [split2(x) for x in inv]
        left = [square_mm(parts[b], [p * mask for p in low_parts[b]]) for b in group]
        left = [split2(x) for x in left]
        inv = [inv[b] - square_mm(left[b], parts[b]) for b in group]
    for_u = [inv[b] * beta_row[b] for b in group]
    for_w = [split2(for_u[b] * (grow_row[b] * nk_row[b])) for b in group]
    for_u = [split2(x) for x in for_u]
    w = [dot(lanes(*for_w[b]), rows(keys[b], keys[b])) for b in group]
    values = [kv_ref[b, :N, N:] for b in group]
    u = [dot(lanes(*for_u[b]), rows(values[b], values[b])) for b in group]
    wu = [lanes(w[b], u[b]) for b in group]
    for b in group:
        wu_hi_ref[b], wu_lo_ref[b] = split2(wu[b])
    save(1)
    save(2)
    last = [x[N - 1 : N, :] for x in cum]
    tail = [jnp.exp(last[b] - cum[b]) * nk_col[b] for b in group]
    faded = [split2(wu[b] * lanes(tail[b], tail[b])) for b in group]
    key_t = [k.T for k in keys]
    out = [dot(lanes(key_t[b], key_t[b]), rows(*faded[b])) for b in group]
    pairs = [lanes(eye * jnp.exp(last[b]) - out[b][:, :N], out[b][:, N:]) for b in group]
    spot = 0
    while len(pairs) > 1:
        for i in range(0, len(pairs), 2):
            node_ref[spot + i // 2] = pairs[i]
        save(4, spot, len(pairs) // 2)
        spot += len(pairs) // 2
        pairs = [compose(pairs[i + 1], pairs[i]) for i in range(0, len(pairs), 2)]
    total_ref[...] = pairs[0]
    for copy in copies:
        copy.wait()


def reach_kernel(kv_ref, qg_ref, gain_ref, *rest):
    sources, (r0_ref, hi_ref, lo_ref, gate_ref) = rest[:5], rest[5:9]
    buffers, sems = rest[9:14], rest[14]
    blocks = kv_ref.shape[0]
    copies = [
        pltpu.make_async_copy(sources[i], buffers[i], sems.at[i]) for i in range(len(sources))
    ]
    for copy in copies:
        copy.start()
    en_ref, wu_hi_ref, wu_lo_ref, grow_ref, node_ref = buffers
    r, c = iotas()
    eye = (r == c).astype(F32)
    for b in range(blocks):
        gate = qg_ref[b, :, N:].astype(F32)
        gate_ref[b] = gate / (1.0 + jnp.exp(-gate)) * gain_ref[...]
    copies[0].wait()
    mixing = [
        split2(en_ref[b] * dot_nt(qg_ref[b, :, :N], kv_ref[b, :N, :N])) for b in range(blocks)
    ]
    copies[1].wait()
    copies[2].wait()
    mixed = [wide_mm(mixing[b], wu_hi_ref[b], wu_lo_ref[b]) for b in range(blocks)]
    copies[3].wait()
    copies[4].wait()
    carried = {}
    base, width = {1: 0}, 1
    while width * 2 < blocks:
        base[width * 2] = base[width] + blocks // width // 2
        width *= 2
    step = blocks // 2
    while step:
        for b in range(step, blocks, 2 * step):
            node = node_ref[base[step] + (b - step) // step // 2]
            carried[b] = compose(node, carried[b - step]) if b > step else node
        step //= 2
    for b in range(blocks):
        q32 = qg_ref[b, :, :N].astype(F32)
        scale = lax.rsqrt(jnp.sum(q32 * q32, axis=1, keepdims=True) + EPS) * N**-0.5
        grow_col = jnp.sum(eye * grow_ref[b, 0:1, :], axis=1, keepdims=True)
        reach = grow_col * q32 - mixed[b][:, :N]
        local = mixed[b][:, N:]
        if b:
            high, low = split2(carried[b])
            out = wide_mm(split2(reach), high, low)
            reach, local = out[:, :N], local + out[:, N:]
        r0_ref[b] = local * scale
        hi_ref[b], lo_ref[b] = split2(reach * scale)


def advance(left, right, extra):
    return square_mm(split2(left), split2(right)) + extra


def pair_kernel(core_ref, own_ref, got_ref, out_ref):
    first = core_ref[0] == 0
    own = own_ref[:, :N]
    left = jnp.where(first, got_ref[:, :N], own)
    right = jnp.where(first, own, got_ref[:, N:])
    out_ref[...] = advance(left, right, jnp.where(first, 0.0, own_ref[:, N:]))


def join_kernel(core_ref, near_ref, map_ref, far_ref, out_ref):
    first = core_ref[0] == 0
    near = near_ref[...]
    left = jnp.where(first, near, map_ref[...])
    out_ref[...] = advance(left, far_ref[...], jnp.where(first, 0.0, near))


def finish_kernel(core_ref, r0_ref, hi_ref, lo_ref, own_ref, swap_ref, first_ref, gate_ref, *rest):
    *far_refs, out_ref = rest
    first = core_ref[0] == 0
    own = own_ref[...]
    swap = swap_ref[...]
    state = advance(
        jnp.where(first, own, swap), sum(ref[...] for ref in far_refs), jnp.where(first, swap, own)
    )
    state = jnp.where(first, state, advance(first_ref[:, :N], state, first_ref[:, N:]))
    y_both = lanes(*split2(state))
    y_both = rows(y_both, y_both)
    for b in range(r0_ref.shape[0]):
        both = dot(lanes(hi_ref[b], lo_ref[b]), y_both)
        res = r0_ref[b] + both[:, :N] + both[:, N:]
        norm = lax.rsqrt(jnp.mean(res * res, axis=1, keepdims=True) + EPS)
        out_ref[b] = (res * norm * gate_ref[b]).astype(BF16)


def call(kernel, out_shape, inputs, core=None, remote=(), spill=(), sems=0):
    vmem = pl.BlockSpec(memory_space=pltpu.VMEM)
    hbm = pl.BlockSpec(memory_space=pltpu.HBM)
    specs = [vmem] * len(inputs) + [hbm] * len(remote)
    inputs = [*inputs, *(pltpu.with_memory_space_constraint(a, pltpu.HBM) for a in remote)]
    if core is not None:
        specs = [pl.BlockSpec(memory_space=pltpu.SMEM)] + specs
        inputs = [core, *inputs]
    return pl.pallas_call(
        kernel,
        out_shape=[*out_shape, *(pltpu.HBM(o.shape, o.dtype) for o in spill)],
        in_specs=specs,
        out_specs=[vmem] * len(out_shape) + [hbm] * len(spill),
        scratch_shapes=[pltpu.VMEM(o.shape, o.dtype) for o in (*remote, *spill)]
        + ([pltpu.SemaphoreType.DMA((sems,))] if sems else []),
        compiler_params=pltpu.CompilerParams(vmem_limit_bytes=40 * 2**20),
    )(*inputs)


def near(*arrays):
    return [pltpu.with_memory_space_constraint(a, pltpu.VMEM) for a in arrays]


def kept(*dims, dtype=F32):
    return pltpu.VMEM(dims, dtype)


def shape(*dims, dtype=F32):
    return jax.ShapeDtypeStruct(dims, dtype)


def by_head(array):
    return jnp.transpose(array, (1, 0, 2))


def to_heads(array):
    return lax.all_to_all(array, "head", split_axis=0, concat_axis=0, tiled=True)


def layer(queries, keys, values, beta, log_decay, out_gate, norm_gain):
    tokens, heads, _ = values.shape
    z = lax.axis_size("z")
    flat = lambda array: array.reshape(tokens * heads, N)
    (kv,) = call(
        pack_kernel,
        [],
        [],
        remote=[flat(keys), flat(values), beta.T, log_decay.T],
        spill=[shape(heads, tokens + 8, 2 * N, dtype=BF16)],
        sems=15,
    )
    kv = to_heads(kv)
    qg = jnp.concatenate([by_head(queries), by_head(out_gate)], axis=2)
    blocks = kv.shape[0]
    square = kept(N, N)
    wide = kept(N, 2 * N)
    wide16 = shape(blocks, N, 2 * N, dtype=BF16)
    core = lax.axis_index("c").astype(jnp.int32).reshape(1)
    kv, qg = lax.optimization_barrier((kv, qg))
    total, en, wu_hi, wu_lo, grow, nodes = call(
        terms_kernel,
        [wide],
        near(kv),
        spill=[
            shape(blocks, N, N),
            wide16,
            wide16,
            shape(blocks, 8, N),
            shape(blocks - 1, N, 2 * N),
        ],
        sems=8,
    )
    got = lax.ppermute(total, "c", [(0, 1), (1, 0)])
    (window,) = call(pair_kernel, [square], near(total, got), core)

    def up(x, d):
        return lax.ppermute(x, "z", [(i, i + d) for i in range(z - d)])

    def cross(x, d, sources, *routes):
        pairs = [
            (2 * i + source, 2 * (i + d) + target)
            for i in sources
            for source, target in zip(routes[::2], routes[1::2])
        ]
        return lax.ppermute(x, ("z", "c"), pairs)

    span, reach_back = 1, z // 2 + 1
    while span * 2 < z:
        far = up(window, span)
        maps = lax.ppermute(window, "c", [(0, 1)])
        if span * 4 >= z:
            done = range(min(span, z - reach_back))
            fars = [cross(window, reach_back, done, 1, target) for target in (0, 1)]
        elif span * 8 >= z:
            qg, window = lax.optimization_barrier((qg, window))
            qg = to_heads(qg)
        (window,) = call(join_kernel, [square], near(window, maps, far), core)
        span *= 2
    left = range(len(done), z - reach_back)
    fars += [cross(window, reach_back, left, 1, target) for target in (0, 1)]
    own = up(window, 1)
    other = cross(window, 1, range(z - 1), 0, 1, 1, 0)
    cube = kept(blocks, N, N)
    cube16 = kept(blocks, N, N, dtype=BF16)
    r0, r1_hi, r1_lo, gate = call(
        reach_kernel,
        [cube, cube16, cube16, cube],
        [*near(kv, qg), norm_gain.reshape(1, N)],
        remote=[en, wu_hi, wu_lo, grow, nodes],
        sems=5,
    )
    (out,) = call(
        finish_kernel,
        [shape(blocks, N, N, dtype=BF16)],
        near(r0, r1_hi, r1_lo, own, other, got, gate, *fars),
        core,
    )
    return out.reshape(blocks * N, 1, N)


def solution(mesh):
    finer = Mesh(mesh.devices.reshape(-1, 2, mesh.shape["head"]), ("z", "c", "head"))
    tokens = ("z", "c", "head")
    in_specs = (
        P(tokens, None, None),
        P(tokens, None, None),
        P(tokens, None, None),
        P(tokens, None),
        P(tokens, None),
        P(tokens, None, None),
        P(),
    )
    out_specs = P(("z", "c"), "head", None)
    return jax.shard_map(layer, mesh=finer, in_specs=in_specs, out_specs=out_specs, check_vma=False)
```

```python
import jax
import jax.numpy as jnp
from jax import lax
from jax.experimental import pallas as pl
from jax.experimental.pallas import tpu as pltpu
from jax.sharding import Mesh
from jax.sharding import PartitionSpec as P


F32 = jnp.float32
BF16 = jnp.bfloat16
N = 128
EPS = 1e-06
SUB = 16


def dot(a, b):
    return jnp.dot(a, b, preferred_element_type=F32)


def dot_nt(a, b):
    return lax.dot_general(a, b, (((1,), (1,)), ((), ())), preferred_element_type=F32)


def split2(x):
    high = x.astype(BF16)
    return high, (x - high.astype(F32)).astype(BF16)


def lanes(*parts):
    return jnp.concatenate(parts, axis=1)


def rows(*parts):
    return jnp.concatenate(parts, axis=0)


def square_mm(a_parts, b_parts):
    b_both = lanes(*b_parts)
    both = dot(lanes(*a_parts), rows(b_both, b_both))
    return both[:, :N] + both[:, N:]


def wide_mm(a_parts, b_high, b_low):
    return dot(lanes(*a_parts), rows(b_high, b_high)) + dot(a_parts[0], b_low)


def compose(later, earlier):
    high, low = split2(earlier)
    out = wide_mm(split2(later[:, :N]), high, low)
    return out + lanes(jnp.zeros((N, N), F32), later[:, N:])


def iotas():
    return lax.broadcasted_iota(jnp.int32, (N, N), 0), lax.broadcasted_iota(jnp.int32, (N, N), 1)


def pack_kernel(k_hbm, v_hbm, beta_hbm, decay_hbm, out_hbm, k_ref, v_ref, beta_ref, decay_ref, out_ref, sems):
    heads, tokens = out_ref.shape[0], k_ref.shape[0] // out_ref.shape[0]
    span = N * 2 // heads
    quarter = k_ref.shape[0] // 4
    copies = []
    for i in range(4):
        part = pl.ds(quarter * i, quarter)
        for j, (source, target) in enumerate(((k_hbm, k_ref), (v_hbm, v_ref))):
            copies.append(
                pltpu.make_async_copy(source.at[part], target.at[part], sems.at[2 * i + j])
            )
            copies[-1].start()
    for i, (source, target) in enumerate(((beta_hbm, beta_ref), (decay_hbm, decay_ref))):
        copies.append(pltpu.make_async_copy(source, target, sems.at[8 + i]))
        copies[-1].start()

    def send(first, count):
        part = pl.ds(first, count)
        copies.append(
            pltpu.make_async_copy(
                out_ref.at[:, part, :], out_hbm.at[:, part, :], sems.at[len(copies)]
            )
        )
        copies[-1].start()

    shape2 = (2 * N, 2 * N)
    r = lax.broadcasted_iota(jnp.int32, shape2, 0)
    c = lax.broadcasted_iota(jnp.int32, shape2, 1)
    order = (c == r % span * heads + r // span).astype(F32).astype(BF16)
    for i in range(tokens // span):
        part = pl.ds(2 * N * i, 2 * N)
        if 2 * N * i % quarter == 0:
            copies[2 * N * i // quarter * 2].wait()
            copies[2 * N * i // quarter * 2 + 1].wait()
        moved = dot(order, lanes(k_ref[part, :], v_ref[part, :])).astype(BF16)
        for h in range(heads):
            out_ref[h, span * i : span * (i + 1), :] = moved[span * h : span * (h + 1), :]
        if 2 * N * (i + 1) % quarter == 0:
            send(span * (i + 1) - tokens // 4, tokens // 4)
    copies[8].wait()
    copies[9].wait()
    both = lanes(decay_ref[...], beta_ref[...])
    high = both.astype(BF16).astype(F32)
    low = both - high
    row = lax.broadcasted_iota(jnp.int32, (8, 2 * N), 0)
    for h in range(heads):
        aux = jnp.where(row == 0, high[h : h + 1, :], jnp.where(row == 1, low[h : h + 1, :], 0.0))
        out_ref[h, tokens : tokens + 8, :] = aux.astype(BF16)
    send(tokens, 8)
    for copy in copies[10:]:
        copy.wait()


def terms_kernel(kv_ref, total_ref, *rest):
    outs, (en_ref, wu_hi_ref, wu_lo_ref, grow_ref, node_ref), sems = rest[:5], rest[5:10], rest[10]
    blocks = kv_ref.shape[0]
    copies = []

    def save(which, first=0, count=blocks):
        part = pl.ds(first, count)
        copies.append(
            pltpu.make_async_copy(rest[5 + which].at[part], outs[which].at[part], sems.at[len(copies)])
        )
        copies[-1].start()

    r, c = iotas()
    one = lambda cond: cond.astype(F32).astype(BF16)
    lower = one(r >= c)
    eye = (r == c).astype(F32)
    inclusive = r >= c
    strict = r > c
    picks = lanes(one(strict), jnp.ones((N, N), BF16))
    picks = rows(picks, picks)
    lane16 = lax.broadcasted_iota(jnp.int32, (SUB, N), 1)
    row16 = lax.broadcasted_iota(jnp.int32, (SUB, N), 0)
    start16 = (row16 == lane16 % SUB).astype(F32)
    base16 = lane16 // SUB * SUB
    merge_masks = [one((r // m == c // m + 1) & (c // m % 2 == 0)) for m in (16, 32, 64)]
    group = range(blocks)

    keys = [kv_ref[b, :N, :N] for b in group]
    kk = [dot_nt(k, k) for k in keys]
    aux = [kv_ref[b, N : N + 8, :] for b in group]
    summed = [dot(lanes(lower * a[0:1, :N], lower * a[1:2, :N]), picks) for a in aux]
    cum = [s[:, N:] for s in summed]
    beta_row = []
    grow_row = []
    nk_row = []
    nk_col = []
    low = []
    for b in group:
        a = aux[b].astype(F32)
        beta_row.append(a[0:1, N:] + a[1:2, N:])
        grow_row.append(jnp.exp(jnp.sum(eye * cum[b], axis=0, keepdims=True)))
        diag = eye * kk[b]
        nk_row.append(lax.rsqrt(jnp.sum(diag, axis=0, keepdims=True) + EPS))
        nk_col.append(lax.rsqrt(jnp.sum(diag, axis=1, keepdims=True) + EPS))
        beta_col = jnp.sum(eye * beta_row[b], axis=1, keepdims=True)
        fade_n = jnp.exp(summed[b][:, :N]) * nk_row[b]
        en_ref[b] = jnp.where(inclusive, fade_n, 0.0)
        low.append(jnp.where(strict, fade_n * (kk[b] * (beta_col * nk_col[b])), 0.0))
        grow_ref[b] = jnp.broadcast_to(grow_row[b], (8, N))
    save(0)
    save(3)
    inv = []
    for b in group:
        small = sum(
            jnp.where(lane16 // SUB == s, low[b][SUB * s : SUB * (s + 1)], 0.0) for s in range(N // SUB)
        )
        x = start16
        for j in range(SUB - 1):
            col = jnp.take_along_axis(small, base16 + j, axis=1)
            x = x - col * x[j : j + 1, :]
        inv.append(rows(*[jnp.where(lane16 // SUB == s, x, 0.0) for s in range(N // SUB)]))
    low_parts = [split2(x) for x in low]
    for mask in merge_masks:
        parts = [split2(x) for x in inv]
        left = [square_mm(parts[b], [p * mask for p in low_parts[b]]) for b in group]
        left = [split2(x) for x in left]
        inv = [inv[b] - square_mm(left[b], parts[b]) for b in group]
    pairs = [None] * blocks
    part = blocks // 2
    for first in range(0, blocks, part):
        some = range(first, first + part)
        wu = {}
        for b in some:
            for_u = inv[b] * beta_row[b]
            for_w = for_u * (grow_row[b] * nk_row[b])
            value = kv_ref[b, :N, N:]
            w = dot(lanes(*split2(for_w)), rows(keys[b], keys[b]))
            wu[b] = (w, dot(lanes(*split2(for_u)), rows(value, value)))
        for b in some:
            wu[b] = lanes(*wu[b])
            wu_hi_ref[b], wu_lo_ref[b] = split2(wu[b])
        save(1, first, part)
        save(2, first, part)
        out = {}
        for b in some:
            last = cum[b][N - 1 : N, :]
            tail = jnp.exp(last - cum[b]) * nk_col[b]
            key_t = keys[b].T
            faded = split2(wu[b] * lanes(tail, tail))
            out[b] = dot(lanes(key_t, key_t), rows(*faded))
        for b in some:
            last = jnp.exp(cum[b][N - 1 : N, :])
            pairs[b] = lanes(eye * last - out[b][:, :N], out[b][:, N:])
            if b % 2 == 0:
                node_ref[b // 2] = pairs[b]
        save(4, first // 2, part // 2)
    spot = blocks // 2
    pairs = [compose(pairs[i + 1], pairs[i]) for i in range(0, blocks, 2)]
    while len(pairs) > 1:
        for i in range(0, len(pairs), 2):
            node_ref[spot + i // 2] = pairs[i]
        save(4, spot, len(pairs) // 2)
        spot += len(pairs) // 2
        pairs = [compose(pairs[i + 1], pairs[i]) for i in range(0, len(pairs), 2)]
    total_ref[...] = pairs[0]
    for copy in copies:
        copy.wait()


def reach_kernel(kv_ref, qg_ref, gain_ref, *rest):
    sources, (r0_ref, hi_ref, lo_ref, gate_ref) = rest[:5], rest[5:9]
    buffers, sems = rest[9:14], rest[14]
    blocks = kv_ref.shape[0]
    copies = [
        pltpu.make_async_copy(sources[i], buffers[i], sems.at[i]) for i in range(len(sources))
    ]
    for copy in copies:
        copy.start()
    en_ref, wu_hi_ref, wu_lo_ref, grow_ref, node_ref = buffers
    r, c = iotas()
    eye = (r == c).astype(F32)
    for b in range(blocks):
        gate = qg_ref[b, :, N:].astype(F32)
        gate_ref[b] = gate / (1.0 + jnp.exp(-gate)) * gain_ref[...]
    copies[0].wait()
    mixing = [
        split2(en_ref[b] * dot_nt(qg_ref[b, :, :N], kv_ref[b, :N, :N])) for b in range(blocks)
    ]
    copies[1].wait()
    copies[2].wait()
    mixed = [wide_mm(mixing[b], wu_hi_ref[b], wu_lo_ref[b]) for b in range(blocks)]
    copies[3].wait()
    copies[4].wait()
    carried = {}
    base, width = {1: 0}, 1
    while width * 2 < blocks:
        base[width * 2] = base[width] + blocks // width // 2
        width *= 2
    step = blocks // 2
    while step:
        for b in range(step, blocks, 2 * step):
            node = node_ref[base[step] + (b - step) // step // 2]
            carried[b] = compose(node, carried[b - step]) if b > step else node
        step //= 2
    for b in range(blocks):
        q32 = qg_ref[b, :, :N].astype(F32)
        scale = lax.rsqrt(jnp.sum(q32 * q32, axis=1, keepdims=True) + EPS) * N**-0.5
        grow_col = jnp.sum(eye * grow_ref[b, 0:1, :], axis=1, keepdims=True)
        reach = grow_col * q32 - mixed[b][:, :N]
        local = mixed[b][:, N:]
        if b:
            high, low = split2(carried[b])
            out = wide_mm(split2(reach), high, low)
            reach, local = out[:, :N], local + out[:, N:]
        r0_ref[b] = local * scale
        hi_ref[b], lo_ref[b] = split2(reach * scale)


def advance(left, right, extra):
    return square_mm(split2(left), split2(right)) + extra


def pair_kernel(core_ref, own_ref, got_ref, out_ref):
    first = core_ref[0] == 0
    own = own_ref[:, :N]
    left = jnp.where(first, got_ref[:, :N], own)
    right = jnp.where(first, own, got_ref[:, N:])
    out_ref[...] = advance(left, right, jnp.where(first, 0.0, own_ref[:, N:]))


def join_kernel(core_ref, near_ref, map_ref, far_ref, out_ref):
    first = core_ref[0] == 0
    near = near_ref[...]
    left = jnp.where(first, near, map_ref[...])
    out_ref[...] = advance(left, far_ref[...], jnp.where(first, 0.0, near))


def finish_kernel(core_ref, r0_ref, hi_ref, lo_ref, own_ref, swap_ref, first_ref, gate_ref, *rest):
    *far_refs, out_ref = rest
    first = core_ref[0] == 0
    own = own_ref[...]
    swap = swap_ref[...]
    state = advance(
        jnp.where(first, own, swap), sum(ref[...] for ref in far_refs), jnp.where(first, swap, own)
    )
    state = jnp.where(first, state, advance(first_ref[:, :N], state, first_ref[:, N:]))
    y_both = lanes(*split2(state))
    y_both = rows(y_both, y_both)
    for b in range(r0_ref.shape[0]):
        both = dot(lanes(hi_ref[b], lo_ref[b]), y_both)
        res = r0_ref[b] + both[:, :N] + both[:, N:]
        norm = lax.rsqrt(jnp.mean(res * res, axis=1, keepdims=True) + EPS)
        out_ref[b] = (res * norm * gate_ref[b]).astype(BF16)


def call(kernel, out_shape, inputs, core=None, remote=(), spill=(), sems=0):
    vmem = pl.BlockSpec(memory_space=pltpu.VMEM)
    hbm = pl.BlockSpec(memory_space=pltpu.HBM)
    specs = [vmem] * len(inputs) + [hbm] * len(remote)
    inputs = [*inputs, *(pltpu.with_memory_space_constraint(a, pltpu.HBM) for a in remote)]
    if core is not None:
        specs = [pl.BlockSpec(memory_space=pltpu.SMEM)] + specs
        inputs = [core, *inputs]
    return pl.pallas_call(
        kernel,
        out_shape=[*out_shape, *(pltpu.HBM(o.shape, o.dtype) for o in spill)],
        in_specs=specs,
        out_specs=[vmem] * len(out_shape) + [hbm] * len(spill),
        scratch_shapes=[pltpu.VMEM(o.shape, o.dtype) for o in (*remote, *spill)]
        + ([pltpu.SemaphoreType.DMA((sems,))] if sems else []),
        compiler_params=pltpu.CompilerParams(vmem_limit_bytes=40 * 2**20),
    )(*inputs)


def near(*arrays):
    return [pltpu.with_memory_space_constraint(a, pltpu.VMEM) for a in arrays]


def kept(*dims, dtype=F32):
    return pltpu.VMEM(dims, dtype)


def shape(*dims, dtype=F32):
    return jax.ShapeDtypeStruct(dims, dtype)


def by_head(array):
    return jnp.transpose(array, (1, 0, 2))


def to_heads(array):
    return lax.all_to_all(array, "head", split_axis=0, concat_axis=0, tiled=True)


def layer(queries, keys, values, beta, log_decay, out_gate, norm_gain):
    tokens, heads, _ = values.shape
    z = lax.axis_size("z")
    flat = lambda array: array.reshape(tokens * heads, N)
    (kv,) = call(
        pack_kernel,
        [],
        [],
        remote=[flat(keys), flat(values), beta.T, log_decay.T],
        spill=[shape(heads, tokens + 8, 2 * N, dtype=BF16)],
        sems=15,
    )
    kv = to_heads(kv)
    qg = jnp.concatenate([by_head(queries), by_head(out_gate)], axis=2)
    blocks = kv.shape[0]
    square = kept(N, N)
    wide = kept(N, 2 * N)
    wide16 = shape(blocks, N, 2 * N, dtype=BF16)
    core = lax.axis_index("c").astype(jnp.int32).reshape(1)
    kv, qg = lax.optimization_barrier((kv, qg))
    total, en, wu_hi, wu_lo, grow, nodes = call(
        terms_kernel,
        [wide],
        near(kv),
        spill=[
            shape(blocks, N, N),
            wide16,
            wide16,
            shape(blocks, 8, N),
            shape(blocks - 1, N, 2 * N),
        ],
        sems=11,
    )
    got = lax.ppermute(total, "c", [(0, 1), (1, 0)])
    (window,) = call(pair_kernel, [square], near(total, got), core)

    def up(x, d):
        return lax.ppermute(x, "z", [(i, i + d) for i in range(z - d)])

    def cross(x, d, sources, *routes):
        pairs = [
            (2 * i + source, 2 * (i + d) + target)
            for i in sources
            for source, target in zip(routes[::2], routes[1::2])
        ]
        return lax.ppermute(x, ("z", "c"), pairs)

    span, reach_back = 1, z // 2 + 1
    while span * 2 < z:
        far = up(window, span)
        maps = lax.ppermute(window, "c", [(0, 1)])
        if span * 4 >= z:
            done = range(min(span, z - reach_back))
            fars = [cross(window, reach_back, done, 1, target) for target in (0, 1)]
        elif span * 8 >= z:
            qg, window = lax.optimization_barrier((qg, window))
            qg = to_heads(qg)
        (window,) = call(join_kernel, [square], near(window, maps, far), core)
        span *= 2
    left = range(len(done), z - reach_back)
    fars += [cross(window, reach_back, left, 1, target) for target in (0, 1)]
    own = up(window, 1)
    other = cross(window, 1, range(z - 1), 0, 1, 1, 0)
    cube = kept(blocks, N, N)
    cube16 = kept(blocks, N, N, dtype=BF16)
    r0, r1_hi, r1_lo, gate = call(
        reach_kernel,
        [cube, cube16, cube16, cube],
        [*near(kv, qg), norm_gain.reshape(1, N)],
        remote=[en, wu_hi, wu_lo, grow, nodes],
        sems=5,
    )
    (out,) = call(
        finish_kernel,
        [shape(blocks, N, N, dtype=BF16)],
        near(r0, r1_hi, r1_lo, own, other, got, gate, *fars),
        core,
    )
    return out.reshape(blocks * N, 1, N)


def solution(mesh):
    finer = Mesh(mesh.devices.reshape(-1, 2, mesh.shape["head"]), ("z", "c", "head"))
    tokens = ("z", "c", "head")
    in_specs = (
        P(tokens, None, None),
        P(tokens, None, None),
        P(tokens, None, None),
        P(tokens, None),
        P(tokens, None),
        P(tokens, None, None),
        P(),
    )
    out_specs = P(("z", "c"), "head", None)
    return jax.shard_map(layer, mesh=finer, in_specs=in_specs, out_specs=out_specs, check_vma=False)
```

```python
import jax
import jax.numpy as jnp
from jax import lax
from jax.experimental import pallas as pl
from jax.experimental.pallas import tpu as pltpu
from jax.sharding import Mesh
from jax.sharding import PartitionSpec as P


F32 = jnp.float32
BF16 = jnp.bfloat16
N = 128
EPS = 1e-06
SUB = 16


def dot(a, b):
    return jnp.dot(a, b, preferred_element_type=F32)


def dot_nt(a, b):
    return lax.dot_general(a, b, (((1,), (1,)), ((), ())), preferred_element_type=F32)


def split2(x):
    high = x.astype(BF16)
    return high, (x - high.astype(F32)).astype(BF16)


def lanes(*parts):
    return jnp.concatenate(parts, axis=1)


def rows(*parts):
    return jnp.concatenate(parts, axis=0)


def square_mm(a_parts, b_parts):
    b_both = lanes(*b_parts)
    both = dot(lanes(*a_parts), rows(b_both, b_both))
    return both[:, :N] + both[:, N:]


def wide_mm(a_parts, b_high, b_low):
    return dot(lanes(*a_parts), rows(b_high, b_high)) + dot(a_parts[0], b_low)


def compose(later, earlier):
    high, low = split2(earlier)
    out = wide_mm(split2(later[:, :N]), high, low)
    return out + lanes(jnp.zeros((N, N), F32), later[:, N:])


def iotas():
    return lax.broadcasted_iota(jnp.int32, (N, N), 0), lax.broadcasted_iota(jnp.int32, (N, N), 1)


def pack_kernel(k_hbm, v_hbm, beta_hbm, decay_hbm, out_hbm, k_ref, v_ref, beta_ref, decay_ref, out_ref, sems):
    heads, tokens = out_ref.shape[0], k_ref.shape[0] // out_ref.shape[0]
    span = N * 2 // heads
    quarter = k_ref.shape[0] // 4
    copies = []
    for i in range(4):
        part = pl.ds(quarter * i, quarter)
        for j, (source, target) in enumerate(((k_hbm, k_ref), (v_hbm, v_ref))):
            copies.append(
                pltpu.make_async_copy(source.at[part], target.at[part], sems.at[2 * i + j])
            )
            copies[-1].start()
    for i, (source, target) in enumerate(((beta_hbm, beta_ref), (decay_hbm, decay_ref))):
        copies.append(pltpu.make_async_copy(source, target, sems.at[8 + i]))
        copies[-1].start()

    def send(first, count):
        part = pl.ds(first, count)
        copies.append(
            pltpu.make_async_copy(
                out_ref.at[:, part, :], out_hbm.at[:, part, :], sems.at[len(copies)]
            )
        )
        copies[-1].start()

    shape2 = (2 * N, 2 * N)
    r = lax.broadcasted_iota(jnp.int32, shape2, 0)
    c = lax.broadcasted_iota(jnp.int32, shape2, 1)
    order = (c == r % span * heads + r // span).astype(F32).astype(BF16)
    for i in range(tokens // span):
        part = pl.ds(2 * N * i, 2 * N)
        if 2 * N * i % quarter == 0:
            copies[2 * N * i // quarter * 2].wait()
            copies[2 * N * i // quarter * 2 + 1].wait()
        moved = dot(order, lanes(k_ref[part, :], v_ref[part, :])).astype(BF16)
        for h in range(heads):
            out_ref[h, span * i : span * (i + 1), :] = moved[span * h : span * (h + 1), :]
        if 2 * N * (i + 1) % quarter == 0:
            send(span * (i + 1) - tokens // 4, tokens // 4)
    copies[8].wait()
    copies[9].wait()
    both = lanes(decay_ref[...], beta_ref[...])
    high = both.astype(BF16).astype(F32)
    low = both - high
    row = lax.broadcasted_iota(jnp.int32, (8, 2 * N), 0)
    for h in range(heads):
        aux = jnp.where(row == 0, high[h : h + 1, :], jnp.where(row == 1, low[h : h + 1, :], 0.0))
        out_ref[h, tokens : tokens + 8, :] = aux.astype(BF16)
    send(tokens, 8)
    for copy in copies[10:]:
        copy.wait()


def terms_kernel(kv_ref, total_ref, *rest):
    outs, (en_ref, wu_hi_ref, wu_lo_ref, grow_ref, node_ref), sems = rest[:5], rest[5:10], rest[10]
    blocks = kv_ref.shape[0]
    copies = []

    def save(which, first=0, count=blocks):
        part = pl.ds(first, count)
        copies.append(
            pltpu.make_async_copy(rest[5 + which].at[part], outs[which].at[part], sems.at[len(copies)])
        )
        copies[-1].start()

    r, c = iotas()
    one = lambda cond: cond.astype(F32).astype(BF16)
    lower = one(r >= c)
    eye = (r == c).astype(F32)
    inclusive = r >= c
    strict = r > c
    picks = lanes(one(strict), jnp.ones((N, N), BF16))
    picks = rows(picks, picks)
    lane16 = lax.broadcasted_iota(jnp.int32, (SUB, N), 1)
    row16 = lax.broadcasted_iota(jnp.int32, (SUB, N), 0)
    start16 = (row16 == lane16 % SUB).astype(F32)
    base16 = lane16 // SUB * SUB
    merge_masks = [one((r // m == c // m + 1) & (c // m % 2 == 0)) for m in (16, 32, 64)]
    group = range(blocks)

    keys = [kv_ref[b, :N, :N] for b in group]
    kk = [dot_nt(k, k) for k in keys]
    aux = [kv_ref[b, N : N + 8, :] for b in group]
    summed = [dot(lanes(lower * a[0:1, :N], lower * a[1:2, :N]), picks) for a in aux]
    cum = [s[:, N:] for s in summed]
    beta_row = []
    grow_row = []
    nk_row = []
    nk_col = []
    low = []
    for b in group:
        a = aux[b].astype(F32)
        beta_row.append(a[0:1, N:] + a[1:2, N:])
        grow_row.append(jnp.exp(jnp.sum(eye * cum[b], axis=0, keepdims=True)))
        diag = eye * kk[b]
        nk_row.append(lax.rsqrt(jnp.sum(diag, axis=0, keepdims=True) + EPS))
        nk_col.append(lax.rsqrt(jnp.sum(diag, axis=1, keepdims=True) + EPS))
        beta_col = jnp.sum(eye * beta_row[b], axis=1, keepdims=True)
        fade_n = jnp.exp(summed[b][:, :N]) * nk_row[b]
        en_ref[b] = jnp.where(inclusive, fade_n, 0.0)
        low.append(jnp.where(strict, fade_n * (kk[b] * (beta_col * nk_col[b])), 0.0))
        grow_ref[b] = jnp.broadcast_to(grow_row[b], (8, N))
    save(0)
    save(3)
    inv = []
    for b in group:
        small = sum(
            jnp.where(lane16 // SUB == s, low[b][SUB * s : SUB * (s + 1)], 0.0) for s in range(N // SUB)
        )
        x = start16
        for j in range(SUB - 1):
            col = jnp.take_along_axis(small, base16 + j, axis=1)
            x = x - col * x[j : j + 1, :]
        inv.append(rows(*[jnp.where(lane16 // SUB == s, x, 0.0) for s in range(N // SUB)]))
    low_parts = [split2(x) for x in low]
    for mask in merge_masks:
        parts = [split2(x) for x in inv]
        left = [square_mm(parts[b], [p * mask for p in low_parts[b]]) for b in group]
        left = [split2(x) for x in left]
        inv = [inv[b] - square_mm(left[b], parts[b]) for b in group]
    pairs = [None] * blocks
    part = blocks // 2
    for first in range(0, blocks, part):
        some = range(first, first + part)
        wu = {}
        for b in some:
            for_u = inv[b] * beta_row[b]
            for_w = for_u * (grow_row[b] * nk_row[b])
            value = kv_ref[b, :N, N:]
            w = dot(lanes(*split2(for_w)), rows(keys[b], keys[b]))
            wu[b] = (w, dot(lanes(*split2(for_u)), rows(value, value)))
        for b in some:
            wu[b] = lanes(*wu[b])
            wu_hi_ref[b], wu_lo_ref[b] = split2(wu[b])
        save(1, first, part)
        save(2, first, part)
        out = {}
        for b in some:
            last = cum[b][N - 1 : N, :]
            tail = jnp.exp(last - cum[b]) * nk_col[b]
            key_t = keys[b].T
            faded = split2(wu[b] * lanes(tail, tail))
            out[b] = dot(lanes(key_t, key_t), rows(*faded))
        for b in some:
            last = jnp.exp(cum[b][N - 1 : N, :])
            pairs[b] = lanes(eye * last - out[b][:, :N], out[b][:, N:])
            if b % 2 == 0:
                node_ref[b // 2] = pairs[b]
        save(4, first // 2, part // 2)
    spot = blocks // 2
    pairs = [compose(pairs[i + 1], pairs[i]) for i in range(0, blocks, 2)]
    while len(pairs) > 1:
        for i in range(0, len(pairs), 2):
            node_ref[spot + i // 2] = pairs[i]
        save(4, spot, len(pairs) // 2)
        spot += len(pairs) // 2
        pairs = [compose(pairs[i + 1], pairs[i]) for i in range(0, len(pairs), 2)]
    total_ref[...] = pairs[0]
    for copy in copies:
        copy.wait()


def reach_kernel(kv_ref, qg_ref, gain_ref, *rest):
    sources, (r0_ref, hi_ref, lo_ref, gate_ref) = rest[:5], rest[5:9]
    buffers, sems = rest[9:14], rest[14]
    blocks = kv_ref.shape[0]
    copies = [
        pltpu.make_async_copy(sources[i], buffers[i], sems.at[i]) for i in range(len(sources))
    ]
    for copy in copies:
        copy.start()
    en_ref, wu_hi_ref, wu_lo_ref, grow_ref, node_ref = buffers
    r, c = iotas()
    eye = (r == c).astype(F32)
    for b in range(blocks):
        gate = qg_ref[b, :, N:].astype(F32)
        gate_ref[b] = gate / (1.0 + jnp.exp(-gate)) * gain_ref[...]
    copies[0].wait()
    mixing = [
        split2(en_ref[b] * dot_nt(qg_ref[b, :, :N], kv_ref[b, :N, :N])) for b in range(blocks)
    ]
    copies[1].wait()
    copies[2].wait()
    mixed = [wide_mm(mixing[b], wu_hi_ref[b], wu_lo_ref[b]) for b in range(blocks)]
    copies[3].wait()
    copies[4].wait()
    carried = {}
    base, width = {1: 0}, 1
    while width * 2 < blocks:
        base[width * 2] = base[width] + blocks // width // 2
        width *= 2
    step = blocks // 2
    while step:
        for b in range(step, blocks, 2 * step):
            node = node_ref[base[step] + (b - step) // step // 2]
            carried[b] = compose(node, carried[b - step]) if b > step else node
        step //= 2
    for b in range(blocks):
        q32 = qg_ref[b, :, :N].astype(F32)
        scale = lax.rsqrt(jnp.sum(q32 * q32, axis=1, keepdims=True) + EPS) * N**-0.5
        grow_col = jnp.sum(eye * grow_ref[b, 0:1, :], axis=1, keepdims=True)
        reach = grow_col * q32 - mixed[b][:, :N]
        local = mixed[b][:, N:]
        if b:
            high, low = split2(carried[b])
            out = wide_mm(split2(reach), high, low)
            reach, local = out[:, :N], local + out[:, N:]
        r0_ref[b] = local * scale
        hi_ref[b], lo_ref[b] = split2(reach * scale)


def advance(left, right, extra):
    return square_mm(split2(left), split2(right)) + extra


def pair_kernel(core_ref, own_ref, got_ref, out_ref):
    first = core_ref[0] == 0
    own = own_ref[:, :N]
    left = jnp.where(first, got_ref[:, :N], own)
    right = jnp.where(first, own, got_ref[:, N:])
    out_ref[...] = advance(left, right, jnp.where(first, 0.0, own_ref[:, N:]))


def join_kernel(core_ref, near_ref, map_ref, far_ref, out_ref):
    first = core_ref[0] == 0
    near = near_ref[...]
    left = jnp.where(first, near, map_ref[...])
    out_ref[...] = advance(left, far_ref[...], jnp.where(first, 0.0, near))


def finish_kernel(core_ref, r0_ref, hi_ref, lo_ref, own_ref, swap_ref, first_ref, gate_ref, *rest):
    *far_refs, out_ref = rest
    first = core_ref[0] == 0
    own = own_ref[...]
    swap = swap_ref[...]
    state = advance(
        jnp.where(first, own, swap), sum(ref[...] for ref in far_refs), jnp.where(first, swap, own)
    )
    state = jnp.where(first, state, advance(first_ref[:, :N], state, first_ref[:, N:]))
    y_both = lanes(*split2(state))
    y_both = rows(y_both, y_both)
    for b in range(r0_ref.shape[0]):
        both = dot(lanes(hi_ref[b], lo_ref[b]), y_both)
        res = r0_ref[b] + both[:, :N] + both[:, N:]
        norm = lax.rsqrt(jnp.mean(res * res, axis=1, keepdims=True) + EPS)
        out_ref[b] = (res * norm * gate_ref[b]).astype(BF16)


def call(kernel, out_shape, inputs, core=None, remote=(), spill=(), sems=0):
    vmem = pl.BlockSpec(memory_space=pltpu.VMEM)
    hbm = pl.BlockSpec(memory_space=pltpu.HBM)
    specs = [vmem] * len(inputs) + [hbm] * len(remote)
    inputs = [*inputs, *(pltpu.with_memory_space_constraint(a, pltpu.HBM) for a in remote)]
    if core is not None:
        specs = [pl.BlockSpec(memory_space=pltpu.SMEM)] + specs
        inputs = [core, *inputs]
    return pl.pallas_call(
        kernel,
        out_shape=[*out_shape, *(pltpu.HBM(o.shape, o.dtype) for o in spill)],
        in_specs=specs,
        out_specs=[vmem] * len(out_shape) + [hbm] * len(spill),
        scratch_shapes=[pltpu.VMEM(o.shape, o.dtype) for o in (*remote, *spill)]
        + ([pltpu.SemaphoreType.DMA((sems,))] if sems else []),
        compiler_params=pltpu.CompilerParams(vmem_limit_bytes=40 * 2**20),
    )(*inputs)


def near(*arrays):
    return [pltpu.with_memory_space_constraint(a, pltpu.VMEM) for a in arrays]


def kept(*dims, dtype=F32):
    return pltpu.VMEM(dims, dtype)


def shape(*dims, dtype=F32):
    return jax.ShapeDtypeStruct(dims, dtype)


def by_head(array):
    return jnp.transpose(array, (1, 0, 2))


def to_heads(array):
    return lax.all_to_all(array, "head", split_axis=0, concat_axis=0, tiled=True)


def layer(queries, keys, values, beta, log_decay, out_gate, norm_gain):
    tokens, heads, _ = values.shape
    z = lax.axis_size("z")
    flat = lambda array: array.reshape(tokens * heads, N)
    (kv,) = call(
        pack_kernel,
        [],
        [],
        remote=[flat(keys), flat(values), beta.T, log_decay.T],
        spill=[shape(heads, tokens + 8, 2 * N, dtype=BF16)],
        sems=15,
    )
    kv = to_heads(kv)
    qg = jnp.concatenate([by_head(queries), by_head(out_gate)], axis=2)
    blocks = kv.shape[0]
    square = kept(N, N)
    wide = kept(N, 2 * N)
    wide16 = shape(blocks, N, 2 * N, dtype=BF16)
    core = lax.axis_index("c").astype(jnp.int32).reshape(1)
    kv, qg = lax.optimization_barrier((kv, qg))
    total, en, wu_hi, wu_lo, grow, nodes = call(
        terms_kernel,
        [wide],
        near(kv),
        spill=[
            shape(blocks, N, N),
            wide16,
            wide16,
            shape(blocks, 8, N),
            shape(blocks - 1, N, 2 * N),
        ],
        sems=11,
    )
    got = lax.ppermute(total, "c", [(0, 1), (1, 0)])
    (window,) = call(pair_kernel, [square], near(total, got), core)

    def move(x, d, *routes):
        pairs = [
            (2 * i + source, 2 * (i + d) + target)
            for chips, source, target in routes
            for i in chips
        ]
        return lax.ppermute(x, ("z", "c"), pairs)

    span, reach_back = 1, z // 2 + 1
    while span * 2 < z:
        far = move(window, span, (range(span, z - span), 0, 0), (range(z - span), 1, 1))
        maps = move(window, 0, (range(span, z), 0, 1))
        if span * 4 >= z:
            done = range(min(span, z - reach_back))
            fars = [move(window, reach_back, (done, 1, target)) for target in (0, 1)]
        elif span * 8 >= z:
            qg, window = lax.optimization_barrier((qg, window))
            qg = to_heads(qg)
        (window,) = call(join_kernel, [square], near(window, maps, far), core)
        span *= 2
    left = range(len(done), z - reach_back)
    fars += [move(window, reach_back, (left, 1, target)) for target in (0, 1)]
    maps_sent = range(reach_back - 1, z - 1)
    own = move(window, 1, (maps_sent, 0, 0), (range(z - 1), 1, 1))
    other = move(window, 1, (maps_sent, 0, 1), (range(z - 1), 1, 0))
    cube = kept(blocks, N, N)
    cube16 = kept(blocks, N, N, dtype=BF16)
    r0, r1_hi, r1_lo, gate = call(
        reach_kernel,
        [cube, cube16, cube16, cube],
        [*near(kv, qg), norm_gain.reshape(1, N)],
        remote=[en, wu_hi, wu_lo, grow, nodes],
        sems=5,
    )
    (out,) = call(
        finish_kernel,
        [shape(blocks, N, N, dtype=BF16)],
        near(r0, r1_hi, r1_lo, own, other, got, gate, *fars),
        core,
    )
    return out.reshape(blocks * N, 1, N)


def solution(mesh):
    finer = Mesh(mesh.devices.reshape(-1, 2, mesh.shape["head"]), ("z", "c", "head"))
    tokens = ("z", "c", "head")
    in_specs = (
        P(tokens, None, None),
        P(tokens, None, None),
        P(tokens, None, None),
        P(tokens, None),
        P(tokens, None),
        P(tokens, None, None),
        P(),
    )
    out_specs = P(("z", "c"), "head", None)
    return jax.shard_map(layer, mesh=finer, in_specs=in_specs, out_specs=out_specs, check_vma=False)
```
